128 devices in a mesh: section: 4 (over x_lo, core), tok: 32 (over y, z, x_hi).
Axes of the slice: x: 4 (x_hi: 2, x_lo: 2; x = x_hi * 2 + x_lo), y: 4, z: 4, core: 2. Of those that a mesh axis runs over, the one named last changes fastest.
Arguments:
- states: bfloat16 [8, 2048, 4096], P('section', 'tok'), may hold values from -60 to 60
- spans: int32 [2, 2], replicated, may hold values from 0 to 7, as said below
Outputs:
- bridges: float32 [2, 4096, 4096], P(None, 'section', 'tok')
- residuals: float32 [2, 4096, 4096], P(None, 'section', 'tok')
The draws below stay inside these ranges and needn't reach their ends.
Inputs may be any that keep to these rules, and one draw needn't show every extreme that they name: `spans`: each row is (start, end) with end - start at least 2.
All inputs are finite; a program needn't handle non-finite values.
Results may differ from the reference program's by a relative error of at most 0.0093.
Values may be sent and summed in bfloat16 or wider, within the bound.
A program may use at most 64 MiB of HBM per device.

```python
import jax
import jax.numpy as jnp
from jax import lax

WIN = 4096
L_DEV = 2
SPANS = 2
CG_STEPS = 2
LAYERS = 8
TOKENS = 2048


def draw_states(key, part):
    keys = jax.random.split(key, 4)
    position = jnp.arange(WIN, dtype=jnp.float32) / (WIN - 1)
    column_scale = jnp.exp(jnp.log(3.0) * position) * jnp.exp(jax.random.uniform(keys[0], (WIN,), minval=-0.4, maxval=0.4))
    anchor = jax.random.normal(keys[1], (TOKENS, WIN))
    updates = 0.5 * jax.random.normal(keys[2], (LAYERS, TOKENS, WIN))
    row_scale = jnp.exp(jax.random.uniform(keys[3], (TOKENS, 1), minval=-0.3, maxval=0.3))
    stream = anchor[None] + jnp.cumsum(updates, axis=0)
    stream = stream * row_scale[None] * column_scale[None, None]
    return jnp.clip(stream, -60.0, 60.0).astype(jnp.bfloat16)


def draw_spans(key, part):
    keys = jax.random.split(key, 2)
    starts = jax.random.randint(keys[0], (SPANS,), 0, LAYERS - L_DEV)
    extra = jax.random.randint(keys[1], (SPANS,), 0, LAYERS - L_DEV - starts)
    ends = starts + L_DEV + extra
    return jnp.stack([starts, ends], axis=1).astype(jnp.int32)


def setup_inputs(seed: int = 0) -> dict:
    seeds = jax.random.split(jax.random.key(seed), 3)
    return {
        "states": draw_states(jax.random.fold_in(seeds[2], 71), 0),
        "spans": draw_spans(jax.random.fold_in(seeds[2], 71), 0),
    }


RIDGE = 0.25


def reference(states, spans):
    total_rows = states.shape[1]
    scaling = 1.0 / total_rows
    bridges = []
    residuals = []
    for k in range(spans.shape[0]):
        source = lax.dynamic_index_in_dim(states, spans[k, 0], 0, keepdims=False)
        target = lax.dynamic_index_in_dim(states, spans[k, 1], 0, keepdims=False)
        right_side = jnp.dot(source.T, target, preferred_element_type=jnp.float32) * scaling

        def operate(direction):
            direction_low = direction.astype(jnp.bfloat16)
            mapped = jnp.dot(source, direction_low, preferred_element_type=jnp.float32).astype(jnp.bfloat16)
            return jnp.dot(source.T, mapped, preferred_element_type=jnp.float32) * scaling + RIDGE * direction

        bridge = jnp.zeros_like(right_side)
        residual = right_side
        direction = right_side
        squares = jnp.sum(residual * residual)
        for step in range(CG_STEPS):
            image = operate(direction)
            curvature = jnp.sum(direction * image)
            step_size = squares / curvature
            bridge = bridge + step_size * direction
            residual = residual - step_size * image
            if step + 1 < CG_STEPS:
                renewed = jnp.sum(residual * residual)
                direction = residual + (renewed / squares) * direction
                squares = renewed
        bridges.append(bridge)
        residuals.append(residual)
    return jnp.stack(bridges), jnp.stack(residuals)
```

```python
import functools

import jax
import jax.numpy as jnp
from jax import lax
from jax.experimental import pallas as pl
from jax.experimental.pallas import tpu as pltpu
from jax.sharding import Mesh
from jax.sharding import PartitionSpec as P

MESH = pl.DeviceIdType.MESH
AXES = ("xl", "core", "y", "z", "xh")
SECTION = ("xl", "core")
TOK = ("y", "z", "xh")
RIDGE = 0.25
F32 = jnp.float32
BF16 = jnp.bfloat16


def nn(left, right):
    return jnp.dot(left, right, preferred_element_type=F32)


def nt(left, right):
    return lax.dot_general(left, right, (((1,), (1,)), ((), ())), preferred_element_type=F32)


def total(value):
    return jnp.sum(jnp.sum(value, axis=0, keepdims=True), axis=1, keepdims=True)


def kernel(
    spans,
    states,
    out_bridge,
    out_residual,
    keep_x,
    send_x,
    recv_x,
    keep_y,
    send_y,
    recv_y,
    near_x,
    near_y,
    xs,
    y_own,
    y_mid,
    ys,
    yt,
    b_t,
    ab_t,
    ar_own,
    ar_ship,
    low,
    part_out,
    part_in,
    mapped,
    ship_out,
    ship_in,
    tile_out,
    tile_in,
    sum_y,
    sum_z,
    send_sems,
    recv_sems,
):
    b = lax.axis_index("xl")
    c = lax.axis_index("core")
    y = lax.axis_index("y")
    z = lax.axis_index("z")
    h = lax.axis_index("xh")
    tokens, width = xs.shape
    scale = 1.0 / tokens
    rows = states.shape[1]
    half = rows // 2
    part = width // 2
    cols = ys.shape[-1]
    side = cols // 2

    def at(xl=b, core=c, yy=y, zz=z, xh=h):
        return (xl, core, yy, zz, xh)

    def step(value, by):
        return lax.rem(value + by, 4)

    count = [0]
    sent = []

    def message(src, dst, device):
        index = count[0]
        count[0] += 1
        copy = pltpu.make_async_remote_copy(
            src_ref=src,
            dst_ref=dst,
            send_sem=send_sems.at[index],
            recv_sem=recv_sems.at[index],
            device_id=device,
            device_id_type=MESH,
        )
        copy.start()
        sent.append(copy)
        return copy

    other = at(core=1 - c)
    partner = at(xl=1 - b)
    neighbour = at(xl=1 - b, xh=1 - h)
    opposite = at(xh=1 - h)

    barrier = pltpu.get_barrier_semaphore()
    greeted = [partner, neighbour, opposite, other]
    greeted += [at(yy=step(y, d), core=cc) for d in (1, 2, 3) for cc in (c, 1 - c)]
    greeted += [at(zz=step(z, d)) for d in (1, 2, 3)]
    for device in greeted:
        pl.semaphore_signal(barrier, inc=1, device_id=device, device_id_type=MESH)

    section = 2 * b + c

    def mine(k, which, row, count_rows, column, count_columns):
        there = spans[k, which] - 2 * section
        area = (pl.ds(row, count_rows), pl.ds(column, count_columns))
        first = states[(0, *area)]
        second = states[(1, *area)]
        zero = jnp.zeros_like(first)
        return lax.select_n(there == 0, lax.select_n(there == 1, zero, second), first)

    for k in range(2):
        for block in range(2):
            there = pl.ds(block * part, part)
            here = pl.multiple_of((2 * block + c) * part, part)
            away = pl.multiple_of((2 * block + 1 - c) * part, part)
            send_x[k, :, there] = mine(k, 0, 0, rows, away, part)
            keep_x[k, :, there] = mine(k, 0, 0, rows, here, part)
        send_y[k] = mine(k, 1, pl.multiple_of((1 - c) * half, half), half, 0, 2 * width)
        keep_y[k] = mine(k, 1, pl.multiple_of(c * half, half), half, 0, 2 * width)

    pl.semaphore_wait(barrier, len(greeted))

    pair_x = message(send_x, recv_x, other)
    pair_y = message(send_y, recv_y, other)
    pair_x.wait_recv()
    keep_x[...] = keep_x[...] + recv_x[...]
    near = [
        message(keep_x.at[1 - b], near_x.at[0], partner),
        message(keep_x.at[1 - b], near_x.at[1], neighbour),
        message(keep_x.at[b], near_x.at[2], opposite),
    ]
    pair_y.wait_recv()
    keep_y[...] = keep_y[...] + recv_y[...]
    near += [
        message(keep_y.at[1 - b], near_y.at[0], partner),
        message(keep_y.at[1 - b], near_y.at[1], neighbour),
        message(keep_y.at[b], near_y.at[2], opposite),
    ]

    def place(kind, first, second, piece=None):
        p, q = (first, second) if kind == 0 else (second, first)
        start = (kind * 16 + p * 4 + q) * rows
        if piece is None:
            return xs.at[pl.ds(start, rows)]
        return xs.at[pl.ds(start + piece * half, half)]

    def along(kind, leg, by):
        if (leg == 0) == (kind == 0):
            return at(yy=step(y, by % 4))
        return at(zz=step(z, by % 4))

    def spread(kind, first):
        return {
            by: message(
                place(kind, first, 0), place(kind, first, by % 4), along(kind, 1, by)
            )
            for by in (1, -1)
        }

    gathered = [{}, {}]

    def start(kind):
        got = gathered[kind]
        for by in (1, -1):
            got["line", by] = message(place(kind, 0, 0), place(kind, by % 4, 0), along(kind, 0, by))
        got["own"] = spread(kind, 0)

    def line(kind, by):
        got = gathered[kind]
        got["line", by].wait_recv()
        piece = 0 if by == 1 else 1
        got["far", by] = message(
            place(kind, by % 4, 0, piece), place(kind, 2, 0, piece), along(kind, 0, by)
        )
        got["spread", by % 4] = spread(kind, by % 4)

    def onward(kind, first, copies):
        got = gathered[kind]
        for by in (1, -1):
            copies[by].wait_recv()
            piece = 0 if by == 1 else 1
            got["end", first, by] = message(
                place(kind, first, by % 4, piece), place(kind, first, 2, piece), along(kind, 1, by)
            )

    def far(kind):
        got = gathered[kind]
        for by in (1, -1):
            got["far", by].wait_recv()
        got["spread", 2] = spread(kind, 2)

    near[0].wait_recv()
    xs[pl.ds(0, rows), :] = keep_x[b] + near_x[0]
    start(0)
    near[1].wait_recv()
    near[2].wait_recv()
    xs[pl.ds(16 * rows, rows), :] = near_x[1] + near_x[2]
    start(1)

    near[3].wait_recv()
    y_own[0] = keep_y[b] + near_y[0]
    near[4].wait_recv()
    near[5].wait_recv()
    y_own[1] = near_y[1] + near_y[2]
    along_y = []
    for by in (1, 3, 2):
        to = step(y, by)
        columns = pl.ds(pl.multiple_of(to * 4 * cols, 4 * cols), 4 * cols)
        along_y.append(message(y_own.at[:, :, columns], y_mid.at[:, by], at(yy=to)))
    columns = pl.ds(pl.multiple_of(y * 4 * cols, 4 * cols), 4 * cols)
    y_mid[:, 0] = y_own[:, :, columns]

    for kind in (0, 1):
        for by in (1, -1):
            line(kind, by)
    for copy in along_y:
        copy.wait_recv()
    along_z = []
    for by in (1, 3, 2):
        to = step(z, by)
        columns = pl.ds(pl.multiple_of(to * cols, cols), cols)
        along_z.append(message(y_mid.at[:, :, :, columns], ys.at[:, :, by, c], at(zz=to)))
    columns = pl.ds(pl.multiple_of(z * cols, cols), cols)
    ys[:, :, 0, c] = y_mid[:, :, :, columns]
    for kind in (0, 1):
        onward(kind, 0, gathered[kind]["own"])
    for kind in (0, 1):
        far(kind)
    for copy in along_z:
        copy.wait_recv()
    cross = message(ys.at[:, :, :, c], ys.at[:, :, :, c], other)
    for first in (1, 3, 2):
        for kind in (0, 1):
            onward(kind, first, gathered[kind]["spread", first])
    cross.wait_recv()
    yt[...] = ys[...].reshape(tokens, cols).T
    for first in (0, 1, 3, 2):
        for kind in (0, 1):
            for by in (1, -1):
                gathered[kind]["end", first, by].wait_recv()

    size = 256
    zero_row = jnp.zeros((1, size), F32)

    def right_side(j, squares):
        there = pl.ds(pl.multiple_of(j * size, size), size)
        value = nn(yt[...], xs[:, there]) * scale
        b_t[:, there] = value
        low[0, :, there] = value.astype(BF16)
        return squares + jnp.sum(value * value, axis=0, keepdims=True)

    squares = lax.fori_loop(0, width // size, right_side, zero_row)
    m0 = jnp.sum(squares, axis=1, keepdims=True)
    tile_out[0] = jnp.broadcast_to(m0, (8, 128))
    norm = message(tile_out.at[0], tile_in, other)

    def apply(turn):
        copies = []
        for i in range(tokens // size):
            value = nt(low[turn], xs[pl.ds(i * size, size), :])
            part_out[turn, i] = value.astype(BF16)
            copies.append(message(part_out.at[turn, i], part_in.at[turn, i], other))
        squares = zero_row
        for i in range(tokens // size):
            copies[i].wait_recv()
            value = part_out[turn, i].astype(F32) + part_in[turn, i].astype(F32)
            squares = squares + jnp.sum(value * value, axis=0, keepdims=True)
            mapped[:, pl.ds(i * size, size)] = value.astype(BF16)
        return jnp.sum(squares, axis=1, keepdims=True) * scale

    length = apply(0)
    norm.wait_recv()
    chip_norm = m0 + tile_in[0:1, 0:1]
    chip_curvature = length + RIDGE * chip_norm
    some = chip_curvature > 0.0
    guess = jnp.where(some, chip_norm / jnp.where(some, chip_curvature, 1.0), 1.0)

    def first_image(j, sums):
        there = pl.ds(pl.multiple_of(j * size, size), size)
        base = b_t[:, there]
        image = nn(mapped[...], xs[:, there]) * scale + RIDGE * base
        ab_t[:, there] = image
        rest = base - guess * image
        low[1, :, there] = rest.astype(BF16)
        terms = (base * image, image * image, rest * image, rest * rest)
        return tuple(s + jnp.sum(t, axis=0, keepdims=True) for s, t in zip(sums, terms))

    sums = lax.fori_loop(0, width // size, first_image, (zero_row,) * 4)
    m1, m2, cross_term, rest_norm = (jnp.sum(s, axis=1, keepdims=True) for s in sums)

    second = 0.5 * apply(1) + RIDGE * rest_norm
    m3 = (second - 2.0 * cross_term + m1) / (guess * guess)
    row = lax.broadcasted_iota(jnp.int32, (8, 128), 0)
    tile = jnp.zeros((8, 128), F32)
    for i, value in enumerate((m0, m1, m2, m3)):
        tile = jnp.where(row == i, value, tile)
    tile_out[1] = tile
    sum_y[0] = tile
    over_y = []
    for by in range(4):
        for flip in range(2):
            if by or flip:
                core = c if flip == 0 else 1 - c
                over_y.append(
                    message(tile_out.at[1], sum_y.at[2 * by + flip], at(yy=step(y, by), core=core))
                )

    def second_image(side_row, column, target):
        def body(j, _):
            there = pl.ds(pl.multiple_of(column + j * size, size), size)
            line_rows = pl.ds(pl.multiple_of(side_row, side), side)
            base = b_t[line_rows, there] - guess * ab_t[line_rows, there]
            image = nn(mapped[line_rows, :], xs[:, there]) * scale + RIDGE * base
            target[:, pl.ds(pl.multiple_of(j * size, size), size)] = image
            return 0

        lax.fori_loop(0, part // size, body, 0)

    second_image((1 - h) * side, (1 - b) * part, ar_ship)
    for copy in over_y:
        copy.wait_recv()
    tile = jnp.sum(sum_y[...], axis=0)
    tile_out[2] = tile
    sum_z[0] = tile
    over_z = [
        message(tile_out.at[2], sum_z.at[by], at(zz=step(z, by))) for by in (1, 2, 3)
    ]
    second_image(h * side, b * part, ar_own)
    for copy in over_z:
        copy.wait_recv()
    tile = jnp.sum(sum_z[...], axis=0)
    m0, m1, m2, m3 = (tile[i : i + 1, 0:1] for i in range(4))

    size1 = m0 / m1
    renewed = m0 - 2.0 * size1 * m1 + size1 * size1 * m2
    ratio = renewed / m0
    more = 1.0 + ratio
    curvature = more * more * m1 - 2.0 * more * size1 * m2 + size1 * size1 * m3
    size2 = renewed / curvature
    of_rest = size1 / guess
    of_base = more - of_rest

    def block(side_row, column):
        line_rows = pl.ds(pl.multiple_of(side_row, side), side)
        there = pl.ds(pl.multiple_of(column, part), part)
        return b_t[line_rows, there], ab_t[line_rows, there]

    def bridge_of(base, image):
        return (size1 + size2 * more) * base - (size1 * size2) * image

    def residual_of(base, image, rest_image):
        return base - (size1 + size2 * of_base) * image - (size2 * of_rest) * rest_image

    ship_out[0] = bridge_of(*block(h * side, (1 - b) * part)).astype(BF16)
    to_partner = message(ship_out.at[0], ship_in.at[0], partner)
    ship_out[1] = residual_of(*block((1 - h) * side, (1 - b) * part), ar_ship[...]).astype(BF16)
    to_neighbour = message(ship_out.at[1], ship_in.at[1], neighbour)
    base, image = block(h * side, b * part)
    out_bridge[b] = bridge_of(base, image)
    out_residual[b] = residual_of(base, image, ar_own[...])
    to_partner.wait_recv()
    out_bridge[1 - b] = ship_in[0].astype(F32)
    to_neighbour.wait_recv()
    out_residual[1 - b] = ship_in[1].astype(F32)
    for copy in sent:
        copy.wait_send()


MESSAGES = 96


def per_device(states, spans):
    _, rows, features = states.shape
    tokens = rows * 32
    width = features // 2
    cols = features // 16
    half = rows // 2
    vmem = pltpu.VMEM
    out = jax.ShapeDtypeStruct((2, cols // 2, width // 2), F32)
    bridge, residual = pl.pallas_call(
        kernel,
        out_shape=(out, out),
        in_specs=[
            pl.BlockSpec(memory_space=pltpu.SMEM),
            pl.BlockSpec(memory_space=vmem),
        ],
        out_specs=(pl.BlockSpec(memory_space=vmem), pl.BlockSpec(memory_space=vmem)),
        scratch_shapes=[
            vmem((2, rows, width), BF16),
            vmem((2, rows, width), BF16),
            vmem((2, rows, width), BF16),
            vmem((2, half, features), BF16),
            vmem((2, half, features), BF16),
            vmem((2, half, features), BF16),
            vmem((3, rows, width), BF16),
            vmem((3, half, features), BF16),
            vmem((tokens, width), BF16),
            vmem((2, half, features), BF16),
            vmem((2, 4, half, 4 * cols), BF16),
            vmem((2, 4, 4, 2, half, cols), BF16),
            vmem((cols, tokens), BF16),
            vmem((cols, width), F32),
            vmem((cols, width), F32),
            vmem((cols // 2, width // 2), F32),
            vmem((cols // 2, width // 2), F32),
            vmem((2, cols, width), BF16),
            vmem((2, tokens // 256, cols, 256), BF16),
            vmem((2, tokens // 256, cols, 256), BF16),
            vmem((cols, tokens), BF16),
            vmem((2, cols // 2, width // 2), BF16),
            vmem((2, cols // 2, width // 2), BF16),
            vmem((3, 8, 128), F32),
            vmem((8, 128), F32),
            vmem((8, 8, 128), F32),
            vmem((4, 8, 128), F32),
            pltpu.SemaphoreType.DMA((MESSAGES,)),
            pltpu.SemaphoreType.DMA((MESSAGES,)),
        ],
        compiler_params=pltpu.CompilerParams(
            collective_id=0, has_side_effects=True, vmem_limit_bytes=60 * 1024 * 1024
        ),
    )(spans, states)
    return jnp.swapaxes(bridge, 1, 2), jnp.swapaxes(residual, 1, 2)


def solution(mesh):
    split = Mesh(mesh.devices.reshape(2, 2, 4, 4, 2), AXES)
    return jax.shard_map(
        per_device,
        mesh=split,
        in_specs=(P(SECTION, TOK, None), P()),
        out_specs=(P(None, SECTION, TOK), P(None, SECTION, TOK)),
        check_vma=False,
    )
```

```python
import jax
import jax.numpy as jnp
from jax import lax
from jax.experimental import pallas as pl
from jax.experimental.pallas import tpu as pltpu
from jax.sharding import Mesh
from jax.sharding import PartitionSpec as P

MESH = pl.DeviceIdType.MESH
AXES = ("xl", "core", "y", "z", "xh")
SECTION = ("xl", "core")
TOK = ("y", "z", "xh")
RIDGE = 0.25
F32 = jnp.float32
BF16 = jnp.bfloat16


def nn(left, right):
    return jnp.dot(left, right, preferred_element_type=F32)


def kernel(
    spans,
    states,
    out_bridge,
    out_residual,
    keep_x,
    send_x,
    recv_x,
    keep_y,
    send_y,
    recv_y,
    near_x,
    near_y,
    xs,
    y_own,
    y_mid,
    ys,
    yt,
    b_t,
    ab_t,
    ar_own,
    ar_ship,
    far_b,
    far_ab,
    far_ar,
    low,
    part_out,
    part_in,
    mapped,
    tile_out,
    tile_in,
    sum_y,
    sum_z,
    sum_far,
    send_sems,
    recv_sems,
):
    b = lax.axis_index("xl")
    c = lax.axis_index("core")
    y = lax.axis_index("y")
    z = lax.axis_index("z")
    h = lax.axis_index("xh")
    tokens, width = xs.shape
    scale = 1.0 / tokens
    rows = states.shape[1]
    half = rows // 2
    part = width // 2
    cols = ys.shape[-1]
    side = cols // 2

    def at(xl=b, core=c, yy=y, zz=z, xh=h):
        return (xl, core, yy, zz, xh)

    def step(value, by):
        return lax.rem(value + by, 4)

    sent = []

    class Message:
        def __init__(self, src, dst, device):
            index = len(sent)
            self.copy = pltpu.make_async_remote_copy(
                src_ref=src,
                dst_ref=dst,
                send_sem=send_sems.at[index],
                recv_sem=recv_sems.at[index],
                device_id=device,
                device_id_type=MESH,
            )
            self.copy.start()
            self.arrived = False
            sent.append(self)

        def need(self):
            if not self.arrived:
                self.arrived = True
                self.copy.wait_recv()

    other = at(core=1 - c)
    partner = at(xl=1 - b)
    neighbour = at(xl=1 - b, xh=1 - h)
    opposite = at(xh=1 - h)

    barrier = pltpu.get_barrier_semaphore()
    greeted = [partner, neighbour, opposite, other]
    greeted += [at(yy=step(y, d), core=cc) for d in (1, 2, 3) for cc in (c, 1 - c)]
    greeted += [at(xl=xl, zz=step(z, d)) for d in (1, 2, 3) for xl in (b, 1 - b)]
    for device in greeted:
        pl.semaphore_signal(barrier, inc=1, device_id=device, device_id_type=MESH)

    section = 2 * b + c

    def mine(k, which, row, count_rows, column, count_columns):
        there = spans[k, which] - 2 * section
        area = (pl.ds(row, count_rows), pl.ds(column, count_columns))
        first = states[(0, *area)]
        second = states[(1, *area)]
        zero = jnp.zeros_like(first)
        return lax.select_n(there == 0, lax.select_n(there == 1, zero, second), first)

    for k in range(2):
        for block in range(2):
            there = pl.ds(block * part, part)
            here = pl.multiple_of((2 * block + c) * part, part)
            away = pl.multiple_of((2 * block + 1 - c) * part, part)
            send_x[k, :, there] = mine(k, 0, 0, rows, away, part)
            keep_x[k, :, there] = mine(k, 0, 0, rows, here, part)
        send_y[k] = mine(k, 1, pl.multiple_of((1 - c) * half, half), half, 0, 2 * width)
        keep_y[k] = mine(k, 1, pl.multiple_of(c * half, half), half, 0, 2 * width)

    pl.semaphore_wait(barrier, len(greeted))

    pair_far = Message(send_x.at[1 - b], recv_x.at[1 - b], other)
    pair_own = Message(send_x.at[b], recv_x.at[b], other)
    pair_y = Message(send_y, recv_y, other)
    pieces = [pl.ds(piece * half, half) for piece in range(2)]

    def ring(k, slot, device):
        return [
            Message(keep_x.at[k, piece], near_x.at[slot, piece], device) for piece in pieces
        ]

    pair_far.need()
    keep_x[1 - b] = keep_x[1 - b] + recv_x[1 - b]
    from_partner = ring(1 - b, 0, partner)
    from_neighbour = ring(1 - b, 1, neighbour)
    pair_own.need()
    keep_x[b] = keep_x[b] + recv_x[b]
    pair_y.need()
    keep_y[...] = keep_y[...] + recv_y[...]

    quarter = half // 2
    moved = {}

    def place(kind, piece, first, second, sub=None):
        p, q = (first, second) if piece == 0 else (second, first)
        row = (kind * 16 + p * 4 + q) * rows + piece * half
        if sub is None:
            return xs.at[pl.ds(row, half)]
        return xs.at[pl.ds(row + sub * quarter, quarter)]

    def along(piece, leg, by):
        if leg == piece:
            return at(yy=step(y, by % 4))
        return at(zz=step(z, by % 4))

    def spread(kind, piece, first):
        for by in (1, -1):
            moved[kind, piece, first, by] = Message(
                place(kind, piece, first, 0),
                place(kind, piece, first, by % 4),
                along(piece, 1, by),
            )

    def own(kind, piece):
        for by in (1, -1):
            moved[kind, piece, "line", by] = Message(
                place(kind, piece, 0, 0), place(kind, piece, by % 4, 0), along(piece, 0, by)
            )
        spread(kind, piece, 0)

    def line(kind, piece, by):
        moved[kind, piece, "line", by].need()
        sub = 0 if by == 1 else 1
        moved[kind, piece, "far", by] = Message(
            place(kind, piece, by % 4, 0, sub), place(kind, piece, 2, 0, sub), along(piece, 0, by)
        )
        spread(kind, piece, by % 4)

    def far(kind, piece):
        for by in (1, -1):
            moved[kind, piece, "far", by].need()
        spread(kind, piece, 2)

    def onward(kind, piece, first):
        for by in (1, -1):
            moved[kind, piece, first, by].need()
            sub = 0 if by == 1 else 1
            moved[kind, piece, first, "end", by] = Message(
                place(kind, piece, first, by % 4, sub),
                place(kind, piece, first, 2, sub),
                along(piece, 1, by),
            )

    def both(action, kind, *rest):
        for piece in range(2):
            action(kind, piece, *rest)

    def whole(kind, p):
        for by in (1, -1):
            moved[kind, 0, p, by].need()
            moved[kind, 0, p, "end", by].need()
            for first in range(4):
                if p == 2:
                    moved[kind, 1, first, "end", by].need()
                elif p == by % 4:
                    moved[kind, 1, first, by].need()

    size = 256

    def right_part(kind, p, fresh):
        whole(kind, p)
        here = pl.ds((kind * 16 + p * 4) * rows, 4 * rows)
        yt[:, here] = ys[kind, p].reshape(4 * rows, cols).T

        def body(j, _):
            there = pl.ds(pl.multiple_of(j * size, size), size)
            value = nn(yt[:, here], xs[here, there])
            b_t[:, there] = value if fresh else b_t[:, there] + value
            return 0

        lax.fori_loop(0, width // size, body, 0)

    for piece in range(2):
        from_partner[piece].need()
        xs[pieces[piece], :] = keep_x[b, pieces[piece], :] + near_x[0, pieces[piece], :]
        own(0, piece)
        if piece == 0:
            from_opposite = ring(b, 2, opposite)
    for by in (1, -1):
        both(line, 0, by)
    near_target = Message(keep_y.at[1 - b], near_y, partner)
    both(onward, 0, 0)
    for piece in range(2):
        from_neighbour[piece].need()
        from_opposite[piece].need()
        xs[pl.ds(16 * rows + piece * half, half), :] = (
            near_x[1, pieces[piece], :] + near_x[2, pieces[piece], :]
        )
        own(1, piece)
    both(far, 0)

    near_target.need()
    y_own[...] = keep_y[b] + near_y[...]
    along_y = []
    for by in (1, 3, 2):
        to = step(y, by)
        columns = pl.ds(pl.multiple_of(to * 4 * cols, 4 * cols), 4 * cols)
        along_y.append(Message(y_own.at[:, columns], y_mid.at[by], at(yy=to)))
    columns = pl.ds(pl.multiple_of(y * 4 * cols, 4 * cols), 4 * cols)
    y_mid[0] = y_own[:, columns]
    for by in (1, -1):
        both(line, 1, by)
    for first in (1, 3):
        both(onward, 0, first)
    for copy in along_y:
        copy.need()
    along_z = []
    for by in (1, 3, 2):
        to = step(z, by)
        columns = pl.ds(pl.multiple_of(to * cols, cols), cols)
        along_z.append(Message(y_mid.at[:, :, columns], ys.at[0, :, by, c], at(zz=to)))
    columns = pl.ds(pl.multiple_of(z * cols, cols), cols)
    ys[0, :, 0, c] = y_mid[:, :, columns]
    both(onward, 1, 0)
    both(far, 1)
    both(onward, 0, 2)
    for copy in along_z:
        copy.need()
    plane = Message(ys.at[0, :, :, c], ys.at[1, :, :, c], opposite)
    cross = [Message(ys.at[0, :, :, c], ys.at[0, :, :, c], other)]
    for first in (1, 3):
        both(onward, 1, first)
    plane.need()
    cross.append(Message(ys.at[1, :, :, c], ys.at[1, :, :, c], other))
    cross[0].need()
    right_part(0, 0, True)
    both(onward, 1, 2)
    right_part(0, 1, False)
    right_part(0, 3, False)
    cross[1].need()
    right_part(1, 0, False)
    right_part(1, 1, False)
    right_part(1, 3, False)

    last = []
    for kind in range(2):
        whole(kind, 2)
        here = pl.ds((kind * 16 + 8) * rows, 4 * rows)
        yt[:, here] = ys[kind, 2].reshape(4 * rows, cols).T
        last.append(here)
    zero_row = jnp.zeros((1, size), F32)

    def right_side(j, squares):
        there = pl.ds(pl.multiple_of(j * size, size), size)
        value = b_t[:, there]
        for here in last:
            value = value + nn(yt[:, here], xs[here, there])
        value = value * scale
        b_t[:, there] = value
        low[0, there, :] = value.astype(BF16).T
        return squares + jnp.sum(value * value, axis=0, keepdims=True)

    squares = lax.fori_loop(0, width // size, right_side, zero_row)
    m0 = jnp.sum(squares, axis=1, keepdims=True)
    tile_out[0] = jnp.broadcast_to(m0, (8, 128))
    norm = Message(tile_out.at[0], tile_in.at[0], other)

    shipped = (
        (partner, h * side, (1 - b) * part, 0),
        (neighbour, (1 - h) * side, (1 - b) * part + part // 2, part // 2),
    )

    def ship(source, target):
        return [
            Message(
                source.at[
                    pl.ds(pl.multiple_of(row, side), side),
                    pl.ds(pl.multiple_of(column, part // 2), part // 2),
                ],
                target.at[:, pl.ds(start, part // 2)],
                device,
            )
            for device, row, column, start in shipped
        ]

    arriving = ship(b_t, far_b)

    def apply(turn):
        copies = []
        for i in range(tokens // size):
            value = nn(xs[pl.ds(i * size, size), :], low[turn])
            part_out[turn, i] = value.astype(BF16).T
            copies.append(Message(part_out.at[turn, i], part_in.at[turn, i], other))
        squares = zero_row
        for i in range(tokens // size):
            copies[i].need()
            value = part_out[turn, i].astype(F32) + part_in[turn, i].astype(F32)
            squares = squares + jnp.sum(value * value, axis=0, keepdims=True)
            mapped[:, pl.ds(i * size, size)] = value.astype(BF16)
        return jnp.sum(squares, axis=1, keepdims=True) * scale

    length = apply(0)
    norm.need()
    chip_norm = m0 + tile_in[0, 0:1, 0:1]
    chip_curvature = length + RIDGE * chip_norm
    some = chip_curvature > 0.0
    guess = jnp.where(some, chip_norm / jnp.where(some, chip_curvature, 1.0), 1.0)

    def first_image(j, sums):
        there = pl.ds(pl.multiple_of(j * size, size), size)
        base = b_t[:, there]
        image = nn(mapped[...], xs[:, there]) * scale + RIDGE * base
        ab_t[:, there] = image
        rest = base - guess * image
        low[1, there, :] = rest.astype(BF16).T
        terms = (base * image, image * image, rest * image, rest * rest)
        return tuple(s + jnp.sum(t, axis=0, keepdims=True) for s, t in zip(sums, terms))

    sums = lax.fori_loop(0, width // size, first_image, (zero_row,) * 4)
    m1, m2, cross_term, rest_norm = (jnp.sum(s, axis=1, keepdims=True) for s in sums)

    arriving += ship(ab_t, far_ab)
    tile_out[3] = jnp.broadcast_to(guess, (8, 128))
    arriving.append(Message(tile_out.at[3], tile_in.at[1], partner))

    second = 0.5 * apply(1) + RIDGE * rest_norm
    m3 = (second - 2.0 * cross_term + m1) / (guess * guess)
    row = lax.broadcasted_iota(jnp.int32, (8, 128), 0)
    tile = jnp.zeros((8, 128), F32)
    for i, value in enumerate((m0, m1, m2, m3)):
        tile = jnp.where(row == i, value, tile)
    tile_out[1] = tile
    sum_y[0] = tile
    over_y = []
    for by in range(4):
        for flip in range(2):
            if by or flip:
                core = c if flip == 0 else 1 - c
                over_y.append(
                    Message(tile_out.at[1], sum_y.at[2 * by + flip], at(yy=step(y, by), core=core))
                )

    def second_image(side_row, column, blocks, put):
        line_rows = pl.ds(pl.multiple_of(side_row, side), side)
        for j in range(blocks):
            there = pl.ds(pl.multiple_of(column + j * size, size), size)
            base = b_t[line_rows, there] - guess * ab_t[line_rows, there]
            put(j * size, nn(mapped[line_rows, :], xs[:, there]) * scale + RIDGE * base)

    for turn, (device, row, column, start) in enumerate(shipped):

        def put(at_column, value):
            ar_ship[turn, :, at_column : at_column + size] = value.astype(BF16)

        second_image(row, column, part // 2 // size, put)
        arriving.append(
            Message(ar_ship.at[turn], far_ar.at[:, pl.ds(start, part // 2)], device)
        )
    for copy in over_y:
        copy.need()
    tile = jnp.sum(sum_y[...], axis=0)
    tile_out[2] = tile
    sum_z[0] = tile
    over_z = [Message(tile_out.at[2], sum_z.at[by], at(zz=step(z, by))) for by in (1, 2, 3)]
    over_z += [
        Message(tile_out.at[2], sum_far.at[by], at(xl=1 - b, zz=step(z, by)))
        for by in (0, 1, 2, 3)
    ]

    def put_own(at_column, value):
        ar_own[:, at_column : at_column + size] = value

    second_image(h * side, b * part, part // size, put_own)

    def finish(k, sums, guess, base, image, rest_image):
        m0, m1, m2, m3 = (sums[i : i + 1, 0:1] for i in range(4))
        size1 = m0 / m1
        renewed = m0 - 2.0 * size1 * m1 + size1 * size1 * m2
        ratio = renewed / m0
        more = 1.0 + ratio
        curvature = more * more * m1 - 2.0 * more * size1 * m2 + size1 * size1 * m3
        size2 = renewed / curvature
        of_rest = size1 / guess
        of_base = more - of_rest
        out_bridge[k] = (size1 + size2 * more) * base - (size1 * size2) * image
        out_residual[k] = (
            base - (size1 + size2 * of_base) * image - (size2 * of_rest) * rest_image
        )

    for copy in over_z:
        copy.need()
    line_rows = pl.ds(pl.multiple_of(h * side, side), side)
    there = pl.ds(pl.multiple_of(b * part, part), part)
    finish(
        b,
        jnp.sum(sum_z[...], axis=0),
        guess,
        b_t[line_rows, there],
        ab_t[line_rows, there],
        ar_own[...],
    )
    for copy in arriving:
        copy.need()
    finish(
        1 - b,
        jnp.sum(sum_far[...], axis=0),
        tile_in[1, 0:1, 0:1],
        far_b[...],
        far_ab[...],
        far_ar[...].astype(F32),
    )
    for message in sent:
        message.copy.wait_send()


MESSAGES = 144


def per_device(states, spans):
    _, rows, features = states.shape
    tokens = rows * 32
    width = features // 2
    cols = features // 16
    half = rows // 2
    vmem = pltpu.VMEM
    out = jax.ShapeDtypeStruct((2, cols // 2, width // 2), F32)
    bridge, residual = pl.pallas_call(
        kernel,
        out_shape=(out, out),
        in_specs=[
            pl.BlockSpec(memory_space=pltpu.SMEM),
            pl.BlockSpec(memory_space=vmem),
        ],
        out_specs=(pl.BlockSpec(memory_space=vmem), pl.BlockSpec(memory_space=vmem)),
        scratch_shapes=[
            vmem((2, rows, width), BF16),
            vmem((2, rows, width), BF16),
            vmem((2, rows, width), BF16),
            vmem((2, half, features), BF16),
            vmem((2, half, features), BF16),
            vmem((2, half, features), BF16),
            vmem((3, rows, width), BF16),
            vmem((half, features), BF16),
            vmem((tokens, width), BF16),
            vmem((half, features), BF16),
            vmem((4, half, 4 * cols), BF16),
            vmem((2, 4, 4, 2, half, cols), BF16),
            vmem((cols, tokens), BF16),
            vmem((cols, width), F32),
            vmem((cols, width), F32),
            vmem((cols // 2, width // 2), F32),
            vmem((2, cols // 2, width // 4), BF16),
            vmem((cols // 2, width // 2), F32),
            vmem((cols // 2, width // 2), F32),
            vmem((cols // 2, width // 2), BF16),
            vmem((2, width, cols), BF16),
            vmem((2, tokens // 256, cols, 256), BF16),
            vmem((2, tokens // 256, cols, 256), BF16),
            vmem((cols, tokens), BF16),
            vmem((4, 8, 128), F32),
            vmem((2, 8, 128), F32),
            vmem((8, 8, 128), F32),
            vmem((4, 8, 128), F32),
            vmem((4, 8, 128), F32),
            pltpu.SemaphoreType.DMA((MESSAGES,)),
            pltpu.SemaphoreType.DMA((MESSAGES,)),
        ],
        compiler_params=pltpu.CompilerParams(
            collective_id=0, has_side_effects=True, vmem_limit_bytes=44 * 1024 * 1024
        ),
    )(spans, states)
    return jnp.swapaxes(bridge, 1, 2), jnp.swapaxes(residual, 1, 2)


def solution(mesh):
    split = Mesh(mesh.devices.reshape(2, 2, 4, 4, 2), AXES)
    return jax.shard_map(
        per_device,
        mesh=split,
        in_specs=(P(SECTION, TOK, None), P()),
        out_specs=(P(None, SECTION, TOK), P(None, SECTION, TOK)),
        check_vma=False,
    )
```

```python
import jax
import jax.numpy as jnp
from jax import lax
from jax.experimental import pallas as pl
from jax.experimental.pallas import tpu as pltpu
from jax.sharding import Mesh
from jax.sharding import PartitionSpec as P

MESH = pl.DeviceIdType.MESH
AXES = ("xl", "core", "y", "z", "xh")
SECTION = ("xl", "core")
TOK = ("y", "z", "xh")
RIDGE = 0.25
F32 = jnp.float32
BF16 = jnp.bfloat16


def nn(left, right):
    return jnp.dot(left, right, preferred_element_type=F32)


def kernel(
    spans,
    states,
    out_bridge,
    out_residual,
    keep_x,
    send_x,
    recv_x,
    keep_y,
    send_y,
    recv_y,
    near_x,
    near_y,
    xs,
    y_own,
    y_mid,
    ys,
    yt,
    b_t,
    ab_t,
    parts,
    ar_ship,
    far_b,
    far_ab,
    far_ar,
    low,
    part_out,
    part_in,
    mapped,
    tile_out,
    tile_in,
    sum_y,
    sum_z,
    sum_far,
    send_sems,
    recv_sems,
):
    b = lax.axis_index("xl")
    c = lax.axis_index("core")
    y = lax.axis_index("y")
    z = lax.axis_index("z")
    h = lax.axis_index("xh")
    tokens, width = xs.shape
    scale = 1.0 / tokens
    rows = states.shape[1]
    half = rows // 2
    part = width // 2
    cols = ys.shape[-1]
    side = cols // 2

    def at(xl=b, core=c, yy=y, zz=z, xh=h):
        return (xl, core, yy, zz, xh)

    def step(value, by):
        return lax.rem(value + by, 4)

    sent = []

    class Message:
        def __init__(self, src, dst, device):
            index = len(sent)
            self.copy = pltpu.make_async_remote_copy(
                src_ref=src,
                dst_ref=dst,
                send_sem=send_sems.at[index],
                recv_sem=recv_sems.at[index],
                device_id=device,
                device_id_type=MESH,
            )
            self.copy.start()
            self.arrived = False
            sent.append(self)

        def need(self):
            if not self.arrived:
                self.arrived = True
                self.copy.wait_recv()

    other = at(core=1 - c)
    partner = at(xl=1 - b)
    neighbour = at(xl=1 - b, xh=1 - h)
    opposite = at(xh=1 - h)

    barrier = pltpu.get_barrier_semaphore()
    greeted = [partner, neighbour, opposite, other]
    greeted += [at(yy=step(y, d)) for d in (1, 2, 3)]
    greeted += [at(xl=xl, zz=step(z, d)) for d in (1, 2, 3) for xl in (b, 1 - b)]
    for device in greeted:
        pl.semaphore_signal(barrier, inc=1, device_id=device, device_id_type=MESH)

    section = 2 * b + c

    def mine(k, which, row, count_rows, column, count_columns):
        there = spans[k, which] - 2 * section
        area = (pl.ds(row, count_rows), pl.ds(column, count_columns))
        first = states[(0, *area)]
        second = states[(1, *area)]
        zero = jnp.zeros_like(first)
        return lax.select_n(there == 0, lax.select_n(there == 1, zero, second), first)

    for k in range(2):
        for block in range(2):
            there = pl.ds(block * part, part)
            here = pl.multiple_of((2 * block + c) * part, part)
            away = pl.multiple_of((2 * block + 1 - c) * part, part)
            send_x[k, :, there] = mine(k, 0, 0, rows, away, part)
            keep_x[k, :, there] = mine(k, 0, 0, rows, here, part)
        send_y[k] = mine(k, 1, pl.multiple_of((1 - c) * half, half), half, 0, 2 * width)
        keep_y[k] = mine(k, 1, pl.multiple_of(c * half, half), half, 0, 2 * width)

    pl.semaphore_wait(barrier, len(greeted))

    pair_far = Message(send_x.at[1 - b], recv_x.at[1 - b], other)
    pair_own = Message(send_x.at[b], recv_x.at[b], other)
    pair_y = Message(send_y, recv_y, other)
    pieces = [pl.ds(piece * half, half) for piece in range(2)]

    def ring(k, slot, device):
        return [
            Message(keep_x.at[k, piece], near_x.at[slot, piece], device) for piece in pieces
        ]

    pair_far.need()
    keep_x[1 - b] = keep_x[1 - b] + recv_x[1 - b]
    from_partner = ring(1 - b, 0, partner)
    from_neighbour = ring(1 - b, 1, neighbour)
    pair_own.need()
    keep_x[b] = keep_x[b] + recv_x[b]
    pair_y.need()
    keep_y[...] = keep_y[...] + recv_y[...]

    quarter = half // 2
    moved = {}

    def place(kind, piece, first, second, sub=None):
        p, q = (first, second) if piece == 0 else (second, first)
        row = (kind * 16 + p * 4 + q) * rows + piece * half
        if sub is None:
            return xs.at[pl.ds(row, half)]
        return xs.at[pl.ds(row + sub * quarter, quarter)]

    def along(piece, leg, by):
        if leg == piece:
            return at(yy=step(y, by % 4))
        return at(zz=step(z, by % 4))

    def spread(kind, piece, first):
        for by in (1, -1):
            moved[kind, piece, first, by] = Message(
                place(kind, piece, first, 0),
                place(kind, piece, first, by % 4),
                along(piece, 1, by),
            )

    def own(kind, piece):
        for by in (1, -1):
            moved[kind, piece, "line", by] = Message(
                place(kind, piece, 0, 0), place(kind, piece, by % 4, 0), along(piece, 0, by)
            )
        spread(kind, piece, 0)

    def line(kind, piece, by):
        moved[kind, piece, "line", by].need()
        sub = 0 if by == 1 else 1
        moved[kind, piece, "far", by] = Message(
            place(kind, piece, by % 4, 0, sub), place(kind, piece, 2, 0, sub), along(piece, 0, by)
        )
        spread(kind, piece, by % 4)

    def far(kind, piece):
        for by in (1, -1):
            moved[kind, piece, "far", by].need()
        spread(kind, piece, 2)

    def onward(kind, piece, first):
        for by in (1, -1):
            moved[kind, piece, first, by].need()
            sub = 0 if by == 1 else 1
            moved[kind, piece, first, "end", by] = Message(
                place(kind, piece, first, by % 4, sub),
                place(kind, piece, first, 2, sub),
                along(piece, 1, by),
            )

    def across(piece, first):
        for by in (1, -1):
            moved[0, piece, first, "end", by].need()
        moved[1, piece, first, "across"] = Message(
            place(0, piece, first, 2), place(1, piece, first, 2), opposite
        )

    def both(action, kind, *rest):
        for piece in range(2):
            action(kind, piece, *rest)

    def end(kind, piece, first):
        if kind == 1 and first != 2:
            moved[kind, piece, first, "across"].need()
        else:
            for by in (1, -1):
                moved[kind, piece, first, "end", by].need()

    def whole(kind, p):
        for by in (1, -1):
            moved[kind, 0, p, by].need()
        end(kind, 0, p)
        for first in range(4):
            if p == 2:
                end(kind, 1, first)
            elif p:
                moved[kind, 1, first, 1 if p == 1 else -1].need()

    size = 256

    blocks = [pl.ds(j * size, size) for j in range(width // size)]

    def right_part(kind, p, fresh):
        whole(kind, p)
        here = pl.ds((kind * 16 + p * 4) * rows, 4 * rows)
        yt[:, here] = ys[kind, p].reshape(4 * rows, cols).T
        for there in blocks:
            value = nn(yt[:, here], xs[here, there])
            b_t[:, there] = value if fresh else b_t[:, there] + value

    for piece in range(2):
        from_partner[piece].need()
        xs[pieces[piece], :] = keep_x[b, pieces[piece], :] + near_x[0, pieces[piece], :]
        own(0, piece)
        if piece == 0:
            from_opposite = ring(b, 2, opposite)
    for by in (1, -1):
        both(line, 0, by)
    near_target = Message(keep_y.at[1 - b], near_y, partner)
    both(onward, 0, 0)
    for piece in range(2):
        from_neighbour[piece].need()
        from_opposite[piece].need()
        xs[pl.ds(16 * rows + piece * half, half), :] = (
            near_x[1, pieces[piece], :] + near_x[2, pieces[piece], :]
        )
        own(1, piece)
    both(far, 0)

    near_target.need()
    y_own[...] = keep_y[b] + near_y[...]
    along_y = []
    for by in (1, 3, 2):
        to = step(y, by)
        columns = pl.ds(pl.multiple_of(to * 4 * cols, 4 * cols), 4 * cols)
        along_y.append(Message(y_own.at[:, columns], y_mid.at[by], at(yy=to)))
    columns = pl.ds(pl.multiple_of(y * 4 * cols, 4 * cols), 4 * cols)
    y_mid[0] = y_own[:, columns]
    for by in (1, -1):
        both(line, 1, by)
    for first in (1, 3):
        both(onward, 0, first)
    for copy in along_y:
        copy.need()
    along_z = []
    for by in (1, 3, 2):
        to = step(z, by)
        columns = pl.ds(pl.multiple_of(to * cols, cols), cols)
        along_z.append(Message(y_mid.at[:, :, columns], ys.at[0, :, by, c], at(zz=to)))
    columns = pl.ds(pl.multiple_of(z * cols, cols), cols)
    ys[0, :, 0, c] = y_mid[:, :, columns]
    both(far, 1)
    both(onward, 0, 2)
    for piece in range(2):
        across(piece, 0)
    for copy in along_z:
        copy.need()
    plane = Message(ys.at[0, :, :, c], ys.at[1, :, :, c], opposite)
    cross = [Message(ys.at[0, :, :, c], ys.at[0, :, :, c], other)]
    for first in (1, 3):
        for piece in range(2):
            across(piece, first)
    both(onward, 1, 2)
    plane.need()
    cross.append(Message(ys.at[1, :, :, c], ys.at[1, :, :, c], other))
    cross[0].need()
    right_part(0, 0, True)
    right_part(0, 1, False)
    right_part(0, 3, False)
    cross[1].need()
    right_part(1, 0, False)
    right_part(1, 1, False)
    right_part(1, 3, False)

    last = []
    for kind in range(2):
        whole(kind, 2)
        here = pl.ds((kind * 16 + 8) * rows, 4 * rows)
        yt[:, here] = ys[kind, 2].reshape(4 * rows, cols).T
        last.append(here)
    zero_row = jnp.zeros((1, size), F32)

    squares = zero_row
    for there in blocks:
        value = b_t[:, there]
        for here in last:
            value = value + nn(yt[:, here], xs[here, there])
        value = value * scale
        b_t[:, there] = value
        low[0, there, :] = value.astype(BF16).T
        squares = squares + jnp.sum(value * value, axis=0, keepdims=True)
    m0 = jnp.sum(squares, axis=1, keepdims=True)
    tile_out[0] = jnp.broadcast_to(m0, (8, 128))
    norm = Message(tile_out.at[0], tile_in.at[0], other)

    shipped = (
        (partner, h * side, (1 - b) * part, 0),
        (neighbour, (1 - h) * side, (1 - b) * part + part // 2, part // 2),
    )

    def ship(source, target):
        return [
            Message(
                source.at[
                    pl.ds(pl.multiple_of(row, side), side),
                    pl.ds(pl.multiple_of(column, part // 2), part // 2),
                ],
                target.at[:, pl.ds(start, part // 2)],
                device,
            )
            for device, row, column, start in shipped
        ]

    arriving = ship(b_t, far_b)

    long = tokens // 2
    spans_of_tokens = [pl.ds(part_of * long, long) for part_of in range(2)]

    def products(turn):
        copies = []
        for part_of in range(2):
            for i in range(long // size):
                value = nn(xs[pl.ds(part_of * long + i * size, size), :], low[turn])
                part_out[turn, part_of, :, pl.ds(i * size, size)] = value.astype(BF16).T
            copies.append(
                Message(part_out.at[turn, part_of], part_in.at[turn, part_of], other)
            )
        return copies

    def add_up(turn, part_of, squares):
        for i in range(long // size):
            there = pl.ds(i * size, size)
            value = part_out[turn, part_of, :, there].astype(F32)
            value = value + part_in[turn, part_of, :, there].astype(F32)
            squares = squares + jnp.sum(value * value, axis=0, keepdims=True)
            mapped[:, pl.ds(part_of * long + i * size, size)] = value.astype(BF16)
        return squares

    row = lax.broadcasted_iota(jnp.int32, (8, 128), 0)

    def tile_of(values):
        tile = jnp.zeros((8, 128), F32)
        for i, value in enumerate(values):
            tile = jnp.where(row == i, value, tile)
        return tile

    copies = products(0)
    copies[0].need()
    squares = add_up(0, 0, zero_row)
    for there in blocks:
        ab_t[:, there] = nn(mapped[:, spans_of_tokens[0]], xs[spans_of_tokens[0], there])
    copies[1].need()
    squares = add_up(0, 1, squares)
    length = jnp.sum(squares, axis=1, keepdims=True) * scale
    norm.need()
    chip_norm = m0 + tile_in[0, 0:1, 0:1]
    chip_curvature = length + RIDGE * chip_norm
    some = chip_curvature > 0.0
    guess = jnp.where(some, chip_norm / jnp.where(some, chip_curvature, 1.0), 1.0)

    sums = [zero_row] * 4
    for there in blocks:
        base = b_t[:, there]
        image = ab_t[:, there] + nn(mapped[:, spans_of_tokens[1]], xs[spans_of_tokens[1], there])
        image = image * scale + RIDGE * base
        ab_t[:, there] = image
        rest = base - guess * image
        low[1, there, :] = rest.astype(BF16).T
        terms = (base * image, image * image, rest * image, rest * rest)
        sums = [total + jnp.sum(t, axis=0, keepdims=True) for total, t in zip(sums, terms)]
    tile = tile_of([jnp.sum(total, axis=1, keepdims=True) for total in sums])
    tile_out[1] = tile
    pair_sums = Message(tile_out.at[1], tile_in.at[2], other)

    copies = products(1)
    arriving += ship(ab_t, far_ab)
    tile_out[3] = jnp.broadcast_to(guess, (8, 128))
    arriving.append(Message(tile_out.at[3], tile_in.at[1], partner))
    pair_sums.need()
    chip = tile + tile_in[2]
    m1, m2, cross_term, rest_norm = (chip[i : i + 1, 0:1] for i in range(4))
    copies[0].need()
    squares = add_up(1, 0, zero_row)
    copies[1].need()
    squares = add_up(1, 1, squares)
    second = jnp.sum(squares, axis=1, keepdims=True) * scale + RIDGE * rest_norm
    m3 = (second - 2.0 * cross_term + m1) / (guess * guess)
    tile = tile_of((chip_norm, m1, m2, m3))
    tile_out[4] = tile
    sum_y[0] = tile
    over_y = [Message(tile_out.at[4], sum_y.at[by], at(yy=step(y, by))) for by in (1, 2, 3)]

    def second_image(side_row, column, count_blocks, put):
        line_rows = pl.ds(pl.multiple_of(side_row, side), side)
        for j in range(count_blocks):
            there = pl.ds(pl.multiple_of(column + j * size, size), size)
            base = b_t[line_rows, there] - guess * ab_t[line_rows, there]
            put(j * size, nn(mapped[line_rows, :], xs[:, there]) * scale + RIDGE * base)

    for turn, (device, row, column, start) in enumerate(shipped):

        def put(at_column, value):
            ar_ship[turn, :, at_column : at_column + size] = value.astype(BF16)

        second_image(row, column, part // 2 // size, put)
        arriving.append(
            Message(ar_ship.at[turn], far_ar.at[:, pl.ds(start, part // 2)], device)
        )
    for copy in over_y:
        copy.need()
    tile = jnp.sum(sum_y[...], axis=0)
    tile_out[2] = tile
    sum_z[0] = tile
    over_z = [Message(tile_out.at[2], sum_z.at[by], at(zz=step(z, by))) for by in (1, 2, 3)]
    over_z += [
        Message(tile_out.at[2], sum_far.at[by], at(xl=1 - b, zz=step(z, by)))
        for by in (0, 1, 2, 3)
    ]

    line_rows = pl.ds(pl.multiple_of(h * side, side), side)
    there = pl.ds(pl.multiple_of(b * part, part), part)

    def put_own(at_column, value):
        parts[0, 2, pl.ds(at_column, size), :] = value.T

    second_image(h * side, b * part, part // size, put_own)
    parts[0, 0] = b_t[line_rows, there].T
    parts[0, 1] = ab_t[line_rows, there].T
    for copy in arriving:
        copy.need()
    parts[1, 0] = far_b[...].T
    parts[1, 1] = far_ab[...].T
    parts[1, 2] = far_ar[...].astype(F32).T

    def finish(k, sums, guess, which):
        m0, m1, m2, m3 = (sums[i : i + 1, 0:1] for i in range(4))
        size1 = m0 / m1
        renewed = m0 - 2.0 * size1 * m1 + size1 * size1 * m2
        ratio = renewed / m0
        more = 1.0 + ratio
        curvature = more * more * m1 - 2.0 * more * size1 * m2 + size1 * size1 * m3
        size2 = renewed / curvature
        of_rest = size1 / guess
        of_base = more - of_rest
        base, image, rest_image = (parts[which, i] for i in range(3))
        out_bridge[k] = (size1 + size2 * more) * base - (size1 * size2) * image
        out_residual[k] = (
            base - (size1 + size2 * of_base) * image - (size2 * of_rest) * rest_image
        )

    for copy in over_z:
        copy.need()
    finish(b, jnp.sum(sum_z[...], axis=0), guess, 0)
    finish(1 - b, jnp.sum(sum_far[...], axis=0), tile_in[1, 0:1, 0:1], 1)
    for message in sent:
        message.copy.wait_send()


MESSAGES = 144


def per_device(states, spans):
    _, rows, features = states.shape
    tokens = rows * 32
    width = features // 2
    cols = features // 16
    half = rows // 2
    vmem = pltpu.VMEM
    out = jax.ShapeDtypeStruct((2, width // 2, cols // 2), F32)
    return pl.pallas_call(
        kernel,
        out_shape=(out, out),
        in_specs=[
            pl.BlockSpec(memory_space=pltpu.SMEM),
            pl.BlockSpec(memory_space=vmem),
        ],
        out_specs=(pl.BlockSpec(memory_space=vmem), pl.BlockSpec(memory_space=vmem)),
        scratch_shapes=[
            vmem((2, rows, width), BF16),
            vmem((2, rows, width), BF16),
            vmem((2, rows, width), BF16),
            vmem((2, half, features), BF16),
            vmem((2, half, features), BF16),
            vmem((2, half, features), BF16),
            vmem((3, rows, width), BF16),
            vmem((half, features), BF16),
            vmem((tokens, width), BF16),
            vmem((half, features), BF16),
            vmem((4, half, 4 * cols), BF16),
            vmem((2, 4, 4, 2, half, cols), BF16),
            vmem((cols, tokens), BF16),
            vmem((cols, width), F32),
            vmem((cols, width), F32),
            vmem((2, 3, width // 2, cols // 2), F32),
            vmem((2, cols // 2, width // 4), BF16),
            vmem((cols // 2, width // 2), F32),
            vmem((cols // 2, width // 2), F32),
            vmem((cols // 2, width // 2), BF16),
            vmem((2, width, cols), BF16),
            vmem((2, 2, cols, tokens // 2), BF16),
            vmem((2, 2, cols, tokens // 2), BF16),
            vmem((cols, tokens), BF16),
            vmem((5, 8, 128), F32),
            vmem((3, 8, 128), F32),
            vmem((4, 8, 128), F32),
            vmem((4, 8, 128), F32),
            vmem((4, 8, 128), F32),
            pltpu.SemaphoreType.DMA((MESSAGES,)),
            pltpu.SemaphoreType.DMA((MESSAGES,)),
        ],
        compiler_params=pltpu.CompilerParams(
            collective_id=0, has_side_effects=True, vmem_limit_bytes=44 * 1024 * 1024
        ),
    )(spans, states)


def solution(mesh):
    split = Mesh(mesh.devices.reshape(2, 2, 4, 4, 2), AXES)
    return jax.shard_map(
        per_device,
        mesh=split,
        in_specs=(P(SECTION, TOK, None), P()),
        out_specs=(P(None, SECTION, TOK), P(None, SECTION, TOK)),
        check_vma=False,
    )
```

```python
import jax
import jax.numpy as jnp
from jax import lax
from jax.experimental import pallas as pl
from jax.experimental.pallas import tpu as pltpu
from jax.sharding import Mesh
from jax.sharding import PartitionSpec as P

MESH = pl.DeviceIdType.MESH
AXES = ("xl", "core", "y", "z", "xh")
SECTION = ("xl", "core")
TOK = ("y", "z", "xh")
RIDGE = 0.25
F32 = jnp.float32
BF16 = jnp.bfloat16


ORDER = (
    ("opposite",),
    ("target",),
    ("own", 0, 0),
    ("own", 0, 1),
    ("line", 0, 0, -1),
    ("line", 0, 0, 1),
    ("own", 1, 0),
    ("line", 0, 1, -1),
    ("own", 1, 1),
    ("target_y",),
    ("onward", 0, 1, 0, 1),
    ("onward", 0, 0, 0, -1),
    ("onward", 0, 0, 0, 1),
    ("line", 1, 0, -1),
    ("line", 0, 1, 1),
    ("onward", 0, 1, 0, -1),
    ("target_z",),
    ("line", 1, 1, 1),
    ("line", 1, 1, -1),
    ("across", 0, 0),
    ("line", 1, 0, 1),
    ("onward", 0, 1, 3, -1),
    ("onward", 0, 0, 1, 1),
    ("onward", 0, 1, 3, 1),
    ("across", 1, 0),
    ("onward", 0, 0, 1, -1),
    ("far", 1, 1),
    ("far", 0, 1),
    ("far", 0, 0),
    ("target_plane",),
    ("far", 1, 0),
    ("onward", 0, 0, 3, -1),
    ("onward", 1, 0, 3, -1),
    ("across", 0, 1),
    ("onward", 1, 1, 1, 1),
    ("onward", 0, 1, 1, -1),
    ("onward", 0, 0, 3, 1),
    ("onward", 1, 1, 2, -1),
    ("onward", 0, 0, 2, -1),
    ("onward", 0, 0, 2, 1),
    ("onward", 0, 1, 1, 1),
    ("onward", 1, 1, 2, 1),
    ("onward", 1, 0, 3, 1),
    ("onward", 1, 1, 1, -1),
    ("across", 1, 3),
    ("onward", 0, 1, 2, 1),
    ("target_core",),
    ("onward", 1, 0, 2, 1),
    ("onward", 1, 0, 2, -1),
    ("onward", 0, 1, 2, -1),
)
ACROSS = tuple(step[1:] for step in ORDER if step[0] == "across")


def nn(left, right):
    return jnp.dot(left, right, preferred_element_type=F32)


def kernel(
    spans,
    states,
    out_bridge,
    out_residual,
    keep_x,
    send_x,
    recv_x,
    keep_y,
    send_y,
    recv_y,
    near_x,
    near_y,
    xs,
    y_own,
    y_mid,
    ys,
    yt,
    b_t,
    ab_t,
    parts,
    ar_ship,
    far_b,
    far_ab,
    far_ar,
    low,
    part_out,
    part_in,
    mapped,
    tile_out,
    tile_in,
    sum_y,
    sum_z,
    sum_far,
    send_sems,
    recv_sems,
):
    b = lax.axis_index("xl")
    c = lax.axis_index("core")
    y = lax.axis_index("y")
    z = lax.axis_index("z")
    h = lax.axis_index("xh")
    tokens, width = xs.shape
    scale = 1.0 / tokens
    rows = states.shape[1]
    half = rows // 2
    part = width // 2
    cols = ys.shape[-1]
    side = cols // 2

    def at(xl=b, core=c, yy=y, zz=z, xh=h):
        return (xl, core, yy, zz, xh)

    def step(value, by):
        return lax.rem(value + by, 4)

    sent = []

    class Message:
        def __init__(self, src, dst, device):
            index = len(sent)
            self.copy = pltpu.make_async_remote_copy(
                src_ref=src,
                dst_ref=dst,
                send_sem=send_sems.at[index],
                recv_sem=recv_sems.at[index],
                device_id=device,
                device_id_type=MESH,
            )
            self.copy.start()
            self.arrived = False
            sent.append(self)

        def need(self):
            if not self.arrived:
                self.arrived = True
                self.copy.wait_recv()

    other = at(core=1 - c)
    partner = at(xl=1 - b)
    neighbour = at(xl=1 - b, xh=1 - h)
    opposite = at(xh=1 - h)

    barrier = pltpu.get_barrier_semaphore()
    greeted = [partner, neighbour, opposite, other]
    greeted += [at(yy=step(y, d)) for d in (1, 2, 3)]
    greeted += [at(xl=xl, zz=step(z, d)) for d in (1, 2, 3) for xl in (b, 1 - b)]
    for device in greeted:
        pl.semaphore_signal(barrier, inc=1, device_id=device, device_id_type=MESH)

    section = 2 * b + c

    def mine(k, which, row, count_rows, column, count_columns):
        there = spans[k, which] - 2 * section
        area = (pl.ds(row, count_rows), pl.ds(column, count_columns))
        first = states[(0, *area)]
        second = states[(1, *area)]
        zero = jnp.zeros_like(first)
        return lax.select_n(there == 0, lax.select_n(there == 1, zero, second), first)

    for k in range(2):
        for block in range(2):
            there = pl.ds(block * part, part)
            here = pl.multiple_of((2 * block + c) * part, part)
            away = pl.multiple_of((2 * block + 1 - c) * part, part)
            send_x[k, :, there] = mine(k, 0, 0, rows, away, part)
            keep_x[k, :, there] = mine(k, 0, 0, rows, here, part)
        send_y[k] = mine(k, 1, pl.multiple_of((1 - c) * half, half), half, 0, 2 * width)
        keep_y[k] = mine(k, 1, pl.multiple_of(c * half, half), half, 0, 2 * width)

    pl.semaphore_wait(barrier, len(greeted))

    pair_far = Message(send_x.at[1 - b], recv_x.at[1 - b], other)
    pair_own = Message(send_x.at[b], recv_x.at[b], other)
    pair_y = Message(send_y, recv_y, other)
    pieces = [pl.ds(piece * half, half) for piece in range(2)]

    def ring(k, slot, device):
        return [
            Message(keep_x.at[k, piece], near_x.at[slot, piece], device) for piece in pieces
        ]

    pair_far.need()
    keep_x[1 - b] = keep_x[1 - b] + recv_x[1 - b]
    from_partner = ring(1 - b, 0, partner)
    from_neighbour = ring(1 - b, 1, neighbour)
    pair_own.need()
    keep_x[b] = keep_x[b] + recv_x[b]
    pair_y.need()
    keep_y[...] = keep_y[...] + recv_y[...]

    quarter = half // 2
    moved = {}

    def place(kind, piece, first, second, sub=None):
        p, q = (first, second) if piece == 0 else (second, first)
        row = (kind * 16 + p * 4 + q) * rows + piece * half
        if sub is None:
            return xs.at[pl.ds(row, half)]
        return xs.at[pl.ds(row + sub * quarter, quarter)]

    def along(piece, leg, by):
        if leg == piece:
            return at(yy=step(y, by % 4))
        return at(zz=step(z, by % 4))

    def spread(kind, piece, first):
        for by in (1, -1):
            moved[kind, piece, first, by] = Message(
                place(kind, piece, first, 0),
                place(kind, piece, first, by % 4),
                along(piece, 1, by),
            )

    def own(kind, piece):
        here = pieces[piece]
        target = pl.ds(kind * 16 * rows + piece * half, half)
        if kind == 0:
            from_partner[piece].need()
            xs[target, :] = keep_x[b, here, :] + near_x[0, here, :]
        else:
            from_neighbour[piece].need()
            from_opposite[piece].need()
            xs[target, :] = near_x[1, here, :] + near_x[2, here, :]
        for by in (1, -1):
            moved[kind, piece, "line", by] = Message(
                place(kind, piece, 0, 0), place(kind, piece, by % 4, 0), along(piece, 0, by)
            )
        spread(kind, piece, 0)

    def line(kind, piece, by):
        moved[kind, piece, "line", by].need()
        sub = 0 if by == 1 else 1
        moved[kind, piece, "far", by] = Message(
            place(kind, piece, by % 4, 0, sub), place(kind, piece, 2, 0, sub), along(piece, 0, by)
        )
        spread(kind, piece, by % 4)

    def far(kind, piece):
        for by in (1, -1):
            moved[kind, piece, "far", by].need()
        spread(kind, piece, 2)

    def onward(kind, piece, first, by):
        moved[kind, piece, first, by].need()
        sub = 0 if by == 1 else 1
        moved[kind, piece, first, "end", by] = Message(
            place(kind, piece, first, by % 4, sub),
            place(kind, piece, first, 2, sub),
            along(piece, 1, by),
        )

    def across(piece, first):
        for by in (1, -1):
            moved[0, piece, first, "end", by].need()
        moved[1, piece, first, "across"] = Message(
            place(0, piece, first, 2), place(1, piece, first, 2), opposite
        )

    def end(kind, piece, first):
        if kind == 1 and (piece, first) in ACROSS:
            moved[kind, piece, first, "across"].need()
        else:
            for by in (1, -1):
                moved[kind, piece, first, "end", by].need()

    def whole(kind, p):
        for by in (1, -1):
            moved[kind, 0, p, by].need()
        end(kind, 0, p)
        for first in range(4):
            if p == 2:
                end(kind, 1, first)
            elif p:
                moved[kind, 1, first, 1 if p == 1 else -1].need()

    size = 256

    blocks = [pl.ds(j * size, size) for j in range(width // size)]

    def right_part(kind, p, fresh):
        whole(kind, p)
        here = pl.ds((kind * 16 + p * 4) * rows, 4 * rows)
        yt[:, here] = ys[kind, p].reshape(4 * rows, cols).T
        for there in blocks:
            value = nn(yt[:, here], xs[here, there])
            b_t[:, there] = value if fresh else b_t[:, there] + value

    near_target, along_y, along_z, plane, cross = [], [], [], [], []
    from_opposite = []

    def opposite_ring():
        from_opposite.extend(ring(b, 2, opposite))

    def target():
        near_target.append(Message(keep_y.at[1 - b], near_y, partner))

    def target_y():
        near_target[0].need()
        y_own[...] = keep_y[b] + near_y[...]
        for by in (1, 3, 2):
            to = step(y, by)
            columns = pl.ds(pl.multiple_of(to * 4 * cols, 4 * cols), 4 * cols)
            along_y.append(Message(y_own.at[:, columns], y_mid.at[by], at(yy=to)))
        columns = pl.ds(pl.multiple_of(y * 4 * cols, 4 * cols), 4 * cols)
        y_mid[0] = y_own[:, columns]

    def target_z():
        for copy in along_y:
            copy.need()
        for by in (1, 3, 2):
            to = step(z, by)
            columns = pl.ds(pl.multiple_of(to * cols, cols), cols)
            along_z.append(Message(y_mid.at[:, :, columns], ys.at[0, :, by, c], at(zz=to)))
        columns = pl.ds(pl.multiple_of(z * cols, cols), cols)
        ys[0, :, 0, c] = y_mid[:, :, columns]

    def target_plane():
        for copy in along_z:
            copy.need()
        plane.append(Message(ys.at[0, :, :, c], ys.at[1, :, :, c], opposite))
        cross.append(Message(ys.at[0, :, :, c], ys.at[0, :, :, c], other))

    def target_core():
        plane[0].need()
        cross.append(Message(ys.at[1, :, :, c], ys.at[1, :, :, c], other))

    steps = {
        "own": own,
        "opposite": opposite_ring,
        "line": line,
        "far": far,
        "onward": onward,
        "across": across,
        "target": target,
        "target_y": target_y,
        "target_z": target_z,
        "target_plane": target_plane,
        "target_core": target_core,
    }
    for name, *arguments in ORDER:
        steps[name](*arguments)
    cross[0].need()
    right_part(0, 0, True)
    right_part(0, 1, False)
    right_part(0, 3, False)
    cross[1].need()
    right_part(1, 0, False)
    right_part(1, 1, False)
    right_part(1, 3, False)

    last = []
    for kind in range(2):
        whole(kind, 2)
        here = pl.ds((kind * 16 + 8) * rows, 4 * rows)
        yt[:, here] = ys[kind, 2].reshape(4 * rows, cols).T
        last.append(here)
    zero_row = jnp.zeros((1, size), F32)

    squares = zero_row
    for there in blocks:
        value = b_t[:, there]
        for here in last:
            value = value + nn(yt[:, here], xs[here, there])
        value = value * scale
        b_t[:, there] = value
        low[0, there, :] = value.astype(BF16).T
        squares = squares + jnp.sum(value * value, axis=0, keepdims=True)
    m0 = jnp.sum(squares, axis=1, keepdims=True)
    tile_out[0] = jnp.broadcast_to(m0, (8, 128))
    norm = Message(tile_out.at[0], tile_in.at[0], other)

    shipped = (
        (partner, h * side, (1 - b) * part, 0),
        (neighbour, (1 - h) * side, (1 - b) * part + part // 2, part // 2),
    )

    def ship(source, target):
        return [
            Message(
                source.at[
                    pl.ds(pl.multiple_of(row, side), side),
                    pl.ds(pl.multiple_of(column, part // 2), part // 2),
                ],
                target.at[:, pl.ds(start, part // 2)],
                device,
            )
            for device, row, column, start in shipped
        ]

    arriving = ship(b_t, far_b)

    long = tokens // 2
    spans_of_tokens = [pl.ds(part_of * long, long) for part_of in range(2)]

    def products(turn):
        copies = []
        for part_of in range(2):
            for i in range(long // size):
                value = nn(xs[pl.ds(part_of * long + i * size, size), :], low[turn])
                part_out[turn, part_of, :, pl.ds(i * size, size)] = value.astype(BF16).T
            copies.append(
                Message(part_out.at[turn, part_of], part_in.at[turn, part_of], other)
            )
        return copies

    def add_up(turn, part_of, squares):
        for i in range(long // size):
            there = pl.ds(i * size, size)
            value = part_out[turn, part_of, :, there].astype(F32)
            value = value + part_in[turn, part_of, :, there].astype(F32)
            squares = squares + jnp.sum(value * value, axis=0, keepdims=True)
            mapped[:, pl.ds(part_of * long + i * size, size)] = value.astype(BF16)
        return squares

    row = lax.broadcasted_iota(jnp.int32, (8, 128), 0)

    def tile_of(values):
        tile = jnp.zeros((8, 128), F32)
        for i, value in enumerate(values):
            tile = jnp.where(row == i, value, tile)
        return tile

    copies = products(0)
    copies[0].need()
    squares = add_up(0, 0, zero_row)
    for there in blocks:
        ab_t[:, there] = nn(mapped[:, spans_of_tokens[0]], xs[spans_of_tokens[0], there])
    copies[1].need()
    squares = add_up(0, 1, squares)
    length = jnp.sum(squares, axis=1, keepdims=True) * scale
    norm.need()
    chip_norm = m0 + tile_in[0, 0:1, 0:1]
    chip_curvature = length + RIDGE * chip_norm
    some = chip_curvature > 0.0
    guess = jnp.where(some, chip_norm / jnp.where(some, chip_curvature, 1.0), 1.0)

    sums = [zero_row] * 4
    for there in blocks:
        base = b_t[:, there]
        image = ab_t[:, there] + nn(mapped[:, spans_of_tokens[1]], xs[spans_of_tokens[1], there])
        image = image * scale + RIDGE * base
        ab_t[:, there] = image
        rest = base - guess * image
        low[1, there, :] = rest.astype(BF16).T
        terms = (base * image, image * image, rest * image, rest * rest)
        sums = [total + jnp.sum(t, axis=0, keepdims=True) for total, t in zip(sums, terms)]
    tile = tile_of([jnp.sum(total, axis=1, keepdims=True) for total in sums])
    tile_out[1] = tile
    pair_sums = Message(tile_out.at[1], tile_in.at[2], other)

    copies = products(1)
    arriving += ship(ab_t, far_ab)
    tile_out[3] = jnp.broadcast_to(guess, (8, 128))
    arriving.append(Message(tile_out.at[3], tile_in.at[1], partner))
    pair_sums.need()
    chip = tile + tile_in[2]
    m1, m2, cross_term, rest_norm = (chip[i : i + 1, 0:1] for i in range(4))
    copies[0].need()
    squares = add_up(1, 0, zero_row)
    copies[1].need()
    squares = add_up(1, 1, squares)
    second = jnp.sum(squares, axis=1, keepdims=True) * scale + RIDGE * rest_norm
    m3 = (second - 2.0 * cross_term + m1) / (guess * guess)
    tile = tile_of((chip_norm, m1, m2, m3))
    tile_out[4] = tile
    sum_y[0] = tile
    over_y = [Message(tile_out.at[4], sum_y.at[by], at(yy=step(y, by))) for by in (1, 2, 3)]

    def second_image(side_row, column, count_blocks, put):
        line_rows = pl.ds(pl.multiple_of(side_row, side), side)
        for j in range(count_blocks):
            there = pl.ds(pl.multiple_of(column + j * size, size), size)
            base = b_t[line_rows, there] - guess * ab_t[line_rows, there]
            put(j * size, nn(mapped[line_rows, :], xs[:, there]) * scale + RIDGE * base)

    for turn, (device, row, column, start) in enumerate(shipped):

        def put(at_column, value):
            ar_ship[turn, :, at_column : at_column + size] = value.astype(BF16)

        second_image(row, column, part // 2 // size, put)
        arriving.append(
            Message(ar_ship.at[turn], far_ar.at[:, pl.ds(start, part // 2)], device)
        )
    for copy in over_y:
        copy.need()
    tile = jnp.sum(sum_y[...], axis=0)
    tile_out[2] = tile
    sum_z[0] = tile
    over_z = [Message(tile_out.at[2], sum_z.at[by], at(zz=step(z, by))) for by in (1, 2, 3)]
    over_z += [
        Message(tile_out.at[2], sum_far.at[by], at(xl=1 - b, zz=step(z, by)))
        for by in (0, 1, 2, 3)
    ]

    line_rows = pl.ds(pl.multiple_of(h * side, side), side)
    there = pl.ds(pl.multiple_of(b * part, part), part)

    def put_own(at_column, value):
        parts[0, 2, pl.ds(at_column, size), :] = value.T

    second_image(h * side, b * part, part // size, put_own)
    parts[0, 0] = b_t[line_rows, there].T
    parts[0, 1] = ab_t[line_rows, there].T
    for copy in arriving:
        copy.need()
    parts[1, 0] = far_b[...].T
    parts[1, 1] = far_ab[...].T
    parts[1, 2] = far_ar[...].astype(F32).T

    def finish(k, sums, guess, which):
        m0, m1, m2, m3 = (sums[i : i + 1, 0:1] for i in range(4))
        size1 = m0 / m1
        renewed = m0 - 2.0 * size1 * m1 + size1 * size1 * m2
        ratio = renewed / m0
        more = 1.0 + ratio
        curvature = more * more * m1 - 2.0 * more * size1 * m2 + size1 * size1 * m3
        size2 = renewed / curvature
        of_rest = size1 / guess
        of_base = more - of_rest
        base, image, rest_image = (parts[which, i] for i in range(3))
        out_bridge[k] = (size1 + size2 * more) * base - (size1 * size2) * image
        out_residual[k] = (
            base - (size1 + size2 * of_base) * image - (size2 * of_rest) * rest_image
        )

    for copy in over_z:
        copy.need()
    finish(b, jnp.sum(sum_z[...], axis=0), guess, 0)
    finish(1 - b, jnp.sum(sum_far[...], axis=0), tile_in[1, 0:1, 0:1], 1)
    for message in sent:
        message.copy.wait_send()


MESSAGES = 144


def per_device(states, spans):
    _, rows, features = states.shape
    tokens = rows * 32
    width = features // 2
    cols = features // 16
    half = rows // 2
    vmem = pltpu.VMEM
    out = jax.ShapeDtypeStruct((2, width // 2, cols // 2), F32)
    return pl.pallas_call(
        kernel,
        out_shape=(out, out),
        in_specs=[
            pl.BlockSpec(memory_space=pltpu.SMEM),
            pl.BlockSpec(memory_space=vmem),
        ],
        out_specs=(pl.BlockSpec(memory_space=vmem), pl.BlockSpec(memory_space=vmem)),
        scratch_shapes=[
            vmem((2, rows, width), BF16),
            vmem((2, rows, width), BF16),
            vmem((2, rows, width), BF16),
            vmem((2, half, features), BF16),
            vmem((2, half, features), BF16),
            vmem((2, half, features), BF16),
            vmem((3, rows, width), BF16),
            vmem((half, features), BF16),
            vmem((tokens, width), BF16),
            vmem((half, features), BF16),
            vmem((4, half, 4 * cols), BF16),
            vmem((2, 4, 4, 2, half, cols), BF16),
            vmem((cols, tokens), BF16),
            vmem((cols, width), F32),
            vmem((cols, width), F32),
            vmem((2, 3, width // 2, cols // 2), F32),
            vmem((2, cols // 2, width // 4), BF16),
            vmem((cols // 2, width // 2), F32),
            vmem((cols // 2, width // 2), F32),
            vmem((cols // 2, width // 2), BF16),
            vmem((2, width, cols), BF16),
            vmem((2, 2, cols, tokens // 2), BF16),
            vmem((2, 2, cols, tokens // 2), BF16),
            vmem((cols, tokens), BF16),
            vmem((5, 8, 128), F32),
            vmem((3, 8, 128), F32),
            vmem((4, 8, 128), F32),
            vmem((4, 8, 128), F32),
            vmem((4, 8, 128), F32),
            pltpu.SemaphoreType.DMA((MESSAGES,)),
            pltpu.SemaphoreType.DMA((MESSAGES,)),
        ],
        compiler_params=pltpu.CompilerParams(
            collective_id=0, has_side_effects=True, vmem_limit_bytes=44 * 1024 * 1024
        ),
    )(spans, states)


def solution(mesh):
    split = Mesh(mesh.devices.reshape(2, 2, 4, 4, 2), AXES)
    return jax.shard_map(
        per_device,
        mesh=split,
        in_specs=(P(SECTION, TOK, None), P()),
        out_specs=(P(None, SECTION, TOK), P(None, SECTION, TOK)),
        check_vma=False,
    )
```

```python
import jax
import jax.numpy as jnp
from jax import lax
from jax.experimental import pallas as pl
from jax.experimental.pallas import tpu as pltpu
from jax.sharding import Mesh
from jax.sharding import PartitionSpec as P

MESH = pl.DeviceIdType.MESH
AXES = ("xl", "core", "y", "z", "xh")
SECTION = ("xl", "core")
TOK = ("y", "z", "xh")
RIDGE = 0.25
F32 = jnp.float32
BF16 = jnp.bfloat16


ORDER = (
    ("opposite",),
    ("target",),
    ("own", 0, 0),
    ("own", 0, 1),
    ("line", 0, 0, -1),
    ("line", 0, 0, 1),
    ("own", 1, 0),
    ("line", 0, 1, -1),
    ("own", 1, 1),
    ("target_y",),
    ("onward", 0, 1, 0, 1),
    ("onward", 0, 0, 0, -1),
    ("onward", 0, 0, 0, 1),
    ("line", 1, 0, -1),
    ("line", 0, 1, 1),
    ("onward", 0, 1, 0, -1),
    ("target_z",),
    ("line", 1, 1, 1),
    ("line", 1, 1, -1),
    ("across", 0, 0),
    ("line", 1, 0, 1),
    ("onward", 0, 1, 3, -1),
    ("onward", 0, 0, 1, 1),
    ("onward", 0, 1, 3, 1),
    ("across", 1, 0),
    ("onward", 0, 0, 1, -1),
    ("far", 1, 1),
    ("far", 0, 1),
    ("far", 0, 0),
    ("target_plane",),
    ("far", 1, 0),
    ("onward", 0, 0, 3, -1),
    ("onward", 1, 0, 3, -1),
    ("across", 0, 1),
    ("onward", 1, 1, 1, 1),
    ("onward", 0, 1, 1, -1),
    ("onward", 0, 0, 3, 1),
    ("onward", 1, 1, 2, -1),
    ("onward", 0, 0, 2, -1),
    ("onward", 0, 0, 2, 1),
    ("onward", 0, 1, 1, 1),
    ("onward", 1, 1, 2, 1),
    ("onward", 1, 0, 3, 1),
    ("onward", 1, 1, 1, -1),
    ("across", 1, 3),
    ("onward", 0, 1, 2, 1),
    ("target_core",),
    ("onward", 1, 0, 2, 1),
    ("onward", 1, 0, 2, -1),
    ("onward", 0, 1, 2, -1),
)
ACROSS = tuple(step[1:] for step in ORDER if step[0] == "across")


def nn(left, right):
    return jnp.dot(left, right, preferred_element_type=F32)


def kernel(
    spans,
    states_hbm,
    out_bridge,
    out_residual,
    states,
    keep_x,
    send_x,
    recv_x,
    keep_y,
    send_y,
    recv_y,
    near_x,
    near_y,
    xs,
    y_own,
    y_mid,
    ys,
    yt,
    b_t,
    ab_t,
    parts,
    ar_ship,
    far_b,
    far_ab,
    far_ar,
    low,
    part_out,
    part_in,
    mapped,
    tile_out,
    tile_in,
    sum_y,
    sum_z,
    sum_far,
    send_sems,
    recv_sems,
    load_sem,
):
    load = pltpu.make_async_copy(states_hbm, states, load_sem)
    load.start()
    b = lax.axis_index("xl")
    c = lax.axis_index("core")
    y = lax.axis_index("y")
    z = lax.axis_index("z")
    h = lax.axis_index("xh")
    tokens, width = xs.shape
    scale = 1.0 / tokens
    rows = states.shape[1]
    half = rows // 2
    part = width // 2
    cols = ys.shape[-1]
    side = cols // 2

    def at(xl=b, core=c, yy=y, zz=z, xh=h):
        return (xl, core, yy, zz, xh)

    def step(value, by):
        return lax.rem(value + by, 4)

    sent = []

    class Message:
        def __init__(self, src, dst, device):
            index = len(sent)
            self.copy = pltpu.make_async_remote_copy(
                src_ref=src,
                dst_ref=dst,
                send_sem=send_sems.at[index],
                recv_sem=recv_sems.at[index],
                device_id=device,
                device_id_type=MESH,
            )
            self.copy.start()
            self.arrived = False
            sent.append(self)

        def need(self):
            if not self.arrived:
                self.arrived = True
                self.copy.wait_recv()

    other = at(core=1 - c)
    partner = at(xl=1 - b)
    neighbour = at(xl=1 - b, xh=1 - h)
    opposite = at(xh=1 - h)

    barrier = pltpu.get_barrier_semaphore()
    greeted = [partner, neighbour, opposite, other]
    greeted += [at(yy=step(y, d)) for d in (1, 2, 3)]
    greeted += [at(xl=xl, zz=step(z, d)) for d in (1, 2, 3) for xl in (b, 1 - b)]
    for device in greeted:
        pl.semaphore_signal(barrier, inc=1, device_id=device, device_id_type=MESH)

    load.wait()

    section = 2 * b + c

    def mine(k, which, row, count_rows, column, count_columns):
        there = spans[k, which] - 2 * section
        area = (pl.ds(row, count_rows), pl.ds(column, count_columns))
        first = states[(0, *area)]
        second = states[(1, *area)]
        zero = jnp.zeros_like(first)
        return lax.select_n(there == 0, lax.select_n(there == 1, zero, second), first)

    for k in range(2):
        for block in range(2):
            there = pl.ds(block * part, part)
            here = pl.multiple_of((2 * block + c) * part, part)
            away = pl.multiple_of((2 * block + 1 - c) * part, part)
            send_x[k, :, there] = mine(k, 0, 0, rows, away, part)
            keep_x[k, :, there] = mine(k, 0, 0, rows, here, part)
        send_y[k] = mine(k, 1, pl.multiple_of((1 - c) * half, half), half, 0, 2 * width)
        keep_y[k] = mine(k, 1, pl.multiple_of(c * half, half), half, 0, 2 * width)

    pl.semaphore_wait(barrier, len(greeted))

    quarter = half // 2
    first_rows, later_rows = pl.ds(0, quarter), pl.ds(quarter, rows - quarter)
    pair_far = [
        Message(send_x.at[1 - b, there], recv_x.at[1 - b, there], other)
        for there in (first_rows, later_rows)
    ]
    pair_own = Message(send_x.at[b], recv_x.at[b], other)
    pair_y = Message(send_y, recv_y, other)
    pieces = [pl.ds(piece * half, half) for piece in range(2)]

    quarters = [pl.ds(i * quarter, quarter) for i in range(4)]

    def ring(k, slot, device, parts_of):
        return [
            Message(keep_x.at[k, there], near_x.at[slot, there], device) for there in parts_of
        ]

    from_partner = []
    for copy, there in zip(pair_far, (first_rows, later_rows)):
        copy.need()
        keep_x[1 - b, there] = keep_x[1 - b, there] + recv_x[1 - b, there]
        sent_now = quarters[:1] if there is first_rows else quarters[1:]
        from_partner += ring(1 - b, 0, partner, sent_now)
    from_neighbour = ring(1 - b, 1, neighbour, pieces)
    pair_own.need()
    keep_x[b] = keep_x[b] + recv_x[b]
    pair_y.need()
    keep_y[...] = keep_y[...] + recv_y[...]

    moved = {}

    def place(kind, piece, first, second, sub=None):
        p, q = (first, second) if piece == 0 else (second, first)
        row = (kind * 16 + p * 4 + q) * rows + piece * half
        if sub is None:
            return xs.at[pl.ds(row, half)]
        return xs.at[pl.ds(row + sub * quarter, quarter)]

    def along(piece, leg, by):
        if leg == piece:
            return at(yy=step(y, by % 4))
        return at(zz=step(z, by % 4))

    def spread(kind, piece, first):
        for by in (1, -1):
            moved[kind, piece, first, by] = Message(
                place(kind, piece, first, 0),
                place(kind, piece, first, by % 4),
                along(piece, 1, by),
            )

    class Both:
        def __init__(self, *messages):
            self.messages = messages

        def need(self):
            for message in self.messages:
                message.need()

    def own_part(kind, piece, sub):
        copies = {}
        for leg in (0, 1):
            for by in (1, -1):
                target = (by % 4, 0) if leg == 0 else (0, by % 4)
                copies[leg, by] = Message(
                    place(kind, piece, 0, 0, sub),
                    place(kind, piece, *target, sub),
                    along(piece, leg, by),
                )
        return copies

    def own(kind, piece):
        if kind == 0:
            copies = []
            for sub in range(2):
                there = quarters[2 * piece + sub]
                from_partner[2 * piece + sub].need()
                xs[there, :] = keep_x[b, there, :] + near_x[0, there, :]
                copies.append(own_part(kind, piece, sub))
            copies = {key: Both(copies[0][key], copies[1][key]) for key in copies[0]}
        else:
            here = pieces[piece]
            from_neighbour[piece].need()
            from_opposite[piece].need()
            xs[pl.ds(16 * rows + piece * half, half), :] = near_x[1, here, :] + near_x[2, here, :]
            copies = own_part(kind, piece, None)
        for by in (1, -1):
            moved[kind, piece, "line", by] = copies[0, by]
            moved[kind, piece, 0, by] = copies[1, by]

    def line(kind, piece, by):
        moved[kind, piece, "line", by].need()
        sub = 0 if by == 1 else 1
        moved[kind, piece, "far", by] = Message(
            place(kind, piece, by % 4, 0, sub), place(kind, piece, 2, 0, sub), along(piece, 0, by)
        )
        spread(kind, piece, by % 4)

    def far(kind, piece):
        for by in (1, -1):
            moved[kind, piece, "far", by].need()
        spread(kind, piece, 2)

    def onward(kind, piece, first, by):
        moved[kind, piece, first, by].need()
        sub = 0 if by == 1 else 1
        moved[kind, piece, first, "end", by] = Message(
            place(kind, piece, first, by % 4, sub),
            place(kind, piece, first, 2, sub),
            along(piece, 1, by),
        )

    def across(piece, first):
        for by in (1, -1):
            moved[0, piece, first, "end", by].need()
        moved[1, piece, first, "across"] = Message(
            place(0, piece, first, 2), place(1, piece, first, 2), opposite
        )

    def end(kind, piece, first):
        if kind == 1 and (piece, first) in ACROSS:
            moved[kind, piece, first, "across"].need()
        else:
            for by in (1, -1):
                moved[kind, piece, first, "end", by].need()

    def whole(kind, p):
        for by in (1, -1):
            moved[kind, 0, p, by].need()
        end(kind, 0, p)
        for first in range(4):
            if p == 2:
                end(kind, 1, first)
            elif p:
                moved[kind, 1, first, 1 if p == 1 else -1].need()

    size = 256

    blocks = [pl.ds(j * size, size) for j in range(width // size)]

    def right_part(kind, p, fresh):
        whole(kind, p)
        here = pl.ds((kind * 16 + p * 4) * rows, 4 * rows)
        yt[:, here] = ys[kind, p].reshape(4 * rows, cols).T
        for there in blocks:
            value = nn(yt[:, here], xs[here, there])
            b_t[:, there] = value if fresh else b_t[:, there] + value

    near_target, along_y, along_z, plane, cross = [], [], [], [], []
    from_opposite = []

    def opposite_ring():
        from_opposite.extend(ring(b, 2, opposite, pieces))

    def target():
        near_target.append(Message(keep_y.at[1 - b], near_y, partner))

    def target_y():
        near_target[0].need()
        y_own[...] = keep_y[b] + near_y[...]
        for by in (1, 3, 2):
            to = step(y, by)
            columns = pl.ds(pl.multiple_of(to * 4 * cols, 4 * cols), 4 * cols)
            along_y.append(Message(y_own.at[:, columns], y_mid.at[by], at(yy=to)))
        columns = pl.ds(pl.multiple_of(y * 4 * cols, 4 * cols), 4 * cols)
        y_mid[0] = y_own[:, columns]

    def target_z():
        for copy in along_y:
            copy.need()
        for by in (1, 3, 2):
            to = step(z, by)
            columns = pl.ds(pl.multiple_of(to * cols, cols), cols)
            along_z.append(Message(y_mid.at[:, :, columns], ys.at[0, :, by, c], at(zz=to)))
        columns = pl.ds(pl.multiple_of(z * cols, cols), cols)
        ys[0, :, 0, c] = y_mid[:, :, columns]

    def target_plane():
        for copy in along_z:
            copy.need()
        plane.append(Message(ys.at[0, :, :, c], ys.at[1, :, :, c], opposite))
        cross.append(Message(ys.at[0, :, :, c], ys.at[0, :, :, c], other))

    def target_core():
        plane[0].need()
        cross.append(Message(ys.at[1, :, :, c], ys.at[1, :, :, c], other))

    steps = {
        "own": own,
        "opposite": opposite_ring,
        "line": line,
        "far": far,
        "onward": onward,
        "across": across,
        "target": target,
        "target_y": target_y,
        "target_z": target_z,
        "target_plane": target_plane,
        "target_core": target_core,
    }
    for name, *arguments in ORDER:
        steps[name](*arguments)
    cross[0].need()
    right_part(0, 0, True)
    right_part(0, 1, False)
    right_part(0, 3, False)
    cross[1].need()
    right_part(1, 0, False)
    right_part(1, 1, False)
    right_part(1, 3, False)

    last = []
    for kind in range(2):
        whole(kind, 2)
        here = pl.ds((kind * 16 + 8) * rows, 4 * rows)
        yt[:, here] = ys[kind, 2].reshape(4 * rows, cols).T
        last.append(here)
    zero_row = jnp.zeros((1, size), F32)

    squares = zero_row
    for there in blocks:
        value = b_t[:, there]
        for here in last:
            value = value + nn(yt[:, here], xs[here, there])
        value = value * scale
        b_t[:, there] = value
        low[0, there, :] = value.astype(BF16).T
        squares = squares + jnp.sum(value * value, axis=0, keepdims=True)
    m0 = jnp.sum(squares, axis=1, keepdims=True)
    tile_out[0] = jnp.broadcast_to(m0, (8, 128))
    norm = Message(tile_out.at[0], tile_in.at[0], other)

    shipped = (
        (partner, h * side, (1 - b) * part, 0),
        (neighbour, (1 - h) * side, (1 - b) * part + part // 2, part // 2),
    )

    def ship(source, target):
        return [
            Message(
                source.at[
                    pl.ds(pl.multiple_of(row, side), side),
                    pl.ds(pl.multiple_of(column, part // 2), part // 2),
                ],
                target.at[:, pl.ds(start, part // 2)],
                device,
            )
            for device, row, column, start in shipped
        ]

    arriving = ship(b_t, far_b)

    long = tokens // 4
    token_halves = [pl.ds(i * 2 * long, 2 * long) for i in range(2)]

    def products(turn):
        copies = []
        for part_of in range(4):
            for i in range(long // size):
                value = nn(xs[pl.ds(part_of * long + i * size, size), :], low[turn])
                part_out[turn, part_of, :, pl.ds(i * size, size)] = value.astype(BF16).T
            copies.append(
                Message(part_out.at[turn, part_of], part_in.at[turn, part_of], other)
            )
        return copies

    def add_up(turn, part_of, squares):
        copies[part_of].need()
        for i in range(long // size):
            there = pl.ds(i * size, size)
            value = part_out[turn, part_of, :, there].astype(F32)
            value = value + part_in[turn, part_of, :, there].astype(F32)
            squares = squares + jnp.sum(value * value, axis=0, keepdims=True)
            mapped[:, pl.ds(part_of * long + i * size, size)] = value.astype(BF16)
        return squares

    row = lax.broadcasted_iota(jnp.int32, (8, 128), 0)

    def tile_of(values):
        tile = jnp.zeros((8, 128), F32)
        for i, value in enumerate(values):
            tile = jnp.where(row == i, value, tile)
        return tile

    copies = products(0)
    squares = add_up(0, 1, add_up(0, 0, zero_row))
    for there in blocks:
        ab_t[:, there] = nn(mapped[:, token_halves[0]], xs[token_halves[0], there])
    squares = add_up(0, 3, add_up(0, 2, squares))
    length = jnp.sum(squares, axis=1, keepdims=True) * scale
    norm.need()
    chip_norm = m0 + tile_in[0, 0:1, 0:1]
    chip_curvature = length + RIDGE * chip_norm
    some = chip_curvature > 0.0
    guess = jnp.where(some, chip_norm / jnp.where(some, chip_curvature, 1.0), 1.0)

    sums = [zero_row] * 4
    for there in blocks:
        base = b_t[:, there]
        image = ab_t[:, there] + nn(mapped[:, token_halves[1]], xs[token_halves[1], there])
        image = image * scale + RIDGE * base
        ab_t[:, there] = image
        rest = base - guess * image
        low[1, there, :] = rest.astype(BF16).T
        terms = (base * image, image * image, rest * image, rest * rest)
        sums = [total + jnp.sum(t, axis=0, keepdims=True) for total, t in zip(sums, terms)]
    tile = tile_of([jnp.sum(total, axis=1, keepdims=True) for total in sums])
    tile_out[1] = tile
    pair_sums = Message(tile_out.at[1], tile_in.at[2], other)

    copies = products(1)
    arriving += ship(ab_t, far_ab)
    tile_out[3] = jnp.broadcast_to(guess, (8, 128))
    arriving.append(Message(tile_out.at[3], tile_in.at[1], partner))
    pair_sums.need()
    chip = tile + tile_in[2]
    m1, m2, cross_term, rest_norm = (chip[i : i + 1, 0:1] for i in range(4))
    squares = zero_row
    for part_of in range(4):
        squares = add_up(1, part_of, squares)
    second = jnp.sum(squares, axis=1, keepdims=True) * scale + RIDGE * rest_norm
    m3 = (second - 2.0 * cross_term + m1) / (guess * guess)
    tile = tile_of((chip_norm, m1, m2, m3))
    tile_out[4] = tile
    sum_y[0] = tile
    over_y = [Message(tile_out.at[4], sum_y.at[by], at(yy=step(y, by))) for by in (1, 2, 3)]

    def second_image(side_row, column, count_blocks, put):
        line_rows = pl.ds(pl.multiple_of(side_row, side), side)
        for j in range(count_blocks):
            there = pl.ds(pl.multiple_of(column + j * size, size), size)
            base = b_t[line_rows, there] - guess * ab_t[line_rows, there]
            put(j * size, nn(mapped[line_rows, :], xs[:, there]) * scale + RIDGE * base)

    for turn, (device, row, column, start) in enumerate(shipped):

        def put(at_column, value):
            ar_ship[turn, :, at_column : at_column + size] = value.astype(BF16)

        second_image(row, column, part // 2 // size, put)
        arriving.append(
            Message(ar_ship.at[turn], far_ar.at[:, pl.ds(start, part // 2)], device)
        )
    for copy in over_y:
        copy.need()
    tile = jnp.sum(sum_y[...], axis=0)
    tile_out[2] = tile
    sum_z[0] = tile
    over_z = [Message(tile_out.at[2], sum_z.at[by], at(zz=step(z, by))) for by in (1, 2, 3)]
    over_z += [
        Message(tile_out.at[2], sum_far.at[by], at(xl=1 - b, zz=step(z, by)))
        for by in (0, 1, 2, 3)
    ]

    line_rows = pl.ds(pl.multiple_of(h * side, side), side)
    there = pl.ds(pl.multiple_of(b * part, part), part)

    def put_own(at_column, value):
        parts[0, 2, pl.ds(at_column, size), :] = value.T

    second_image(h * side, b * part, part // size, put_own)
    parts[0, 0] = b_t[line_rows, there].T
    parts[0, 1] = ab_t[line_rows, there].T
    for copy in arriving:
        copy.need()
    parts[1, 0] = far_b[...].T
    parts[1, 1] = far_ab[...].T
    parts[1, 2] = far_ar[...].astype(F32).T

    def finish(k, sums, guess, which):
        m0, m1, m2, m3 = (sums[i : i + 1, 0:1] for i in range(4))
        size1 = m0 / m1
        renewed = m0 - 2.0 * size1 * m1 + size1 * size1 * m2
        ratio = renewed / m0
        more = 1.0 + ratio
        curvature = more * more * m1 - 2.0 * more * size1 * m2 + size1 * size1 * m3
        size2 = renewed / curvature
        of_rest = size1 / guess
        of_base = more - of_rest
        base, image, rest_image = (parts[which, i] for i in range(3))
        out_bridge[k] = (size1 + size2 * more) * base - (size1 * size2) * image
        out_residual[k] = (
            base - (size1 + size2 * of_base) * image - (size2 * of_rest) * rest_image
        )

    for copy in over_z:
        copy.need()
    finish(b, jnp.sum(sum_z[...], axis=0), guess, 0)
    finish(1 - b, jnp.sum(sum_far[...], axis=0), tile_in[1, 0:1, 0:1], 1)
    for message in sent:
        message.copy.wait_send()


MESSAGES = 168


def per_device(states, spans):
    _, rows, features = states.shape
    tokens = rows * 32
    width = features // 2
    cols = features // 16
    half = rows // 2
    vmem = pltpu.VMEM
    out = jax.ShapeDtypeStruct((2, width // 2, cols // 2), F32)
    return pl.pallas_call(
        kernel,
        out_shape=(out, out),
        in_specs=[
            pl.BlockSpec(memory_space=pltpu.SMEM),
            pl.BlockSpec(memory_space=pltpu.HBM),
        ],
        out_specs=(pl.BlockSpec(memory_space=vmem), pl.BlockSpec(memory_space=vmem)),
        scratch_shapes=[
            vmem((2, rows, features), BF16),
            vmem((2, rows, width), BF16),
            vmem((2, rows, width), BF16),
            vmem((2, rows, width), BF16),
            vmem((2, half, features), BF16),
            vmem((2, half, features), BF16),
            vmem((2, half, features), BF16),
            vmem((3, rows, width), BF16),
            vmem((half, features), BF16),
            vmem((tokens, width), BF16),
            vmem((half, features), BF16),
            vmem((4, half, 4 * cols), BF16),
            vmem((2, 4, 4, 2, half, cols), BF16),
            vmem((cols, tokens), BF16),
            vmem((cols, width), F32),
            vmem((cols, width), F32),
            vmem((2, 3, width // 2, cols // 2), F32),
            vmem((2, cols // 2, width // 4), BF16),
            vmem((cols // 2, width // 2), F32),
            vmem((cols // 2, width // 2), F32),
            vmem((cols // 2, width // 2), BF16),
            vmem((2, width, cols), BF16),
            vmem((2, 4, cols, tokens // 4), BF16),
            vmem((2, 4, cols, tokens // 4), BF16),
            vmem((cols, tokens), BF16),
            vmem((5, 8, 128), F32),
            vmem((3, 8, 128), F32),
            vmem((4, 8, 128), F32),
            vmem((4, 8, 128), F32),
            vmem((4, 8, 128), F32),
            pltpu.SemaphoreType.DMA((MESSAGES,)),
            pltpu.SemaphoreType.DMA((MESSAGES,)),
            pltpu.SemaphoreType.DMA,
        ],
        compiler_params=pltpu.CompilerParams(
            collective_id=0, has_side_effects=True, vmem_limit_bytes=51 * 1024 * 1024
        ),
    )(spans, states)


def solution(mesh):
    split = Mesh(mesh.devices.reshape(2, 2, 4, 4, 2), AXES)
    return jax.shard_map(
        per_device,
        mesh=split,
        in_specs=(P(SECTION, TOK, None), P()),
        out_specs=(P(None, SECTION, TOK), P(None, SECTION, TOK)),
        check_vma=False,
    )
```

```python
import jax
import jax.numpy as jnp
from jax import lax
from jax.experimental import pallas as pl
from jax.experimental.pallas import tpu as pltpu
from jax.sharding import Mesh
from jax.sharding import PartitionSpec as P

MESH = pl.DeviceIdType.MESH
AXES = ("xl", "core", "y", "z", "xh")
SECTION = ("xl", "core")
TOK = ("y", "z", "xh")
RIDGE = 0.25
F32 = jnp.float32
BF16 = jnp.bfloat16


ORDER = (
    ("opposite",),
    ("target",),
    ("own", 0, 0),
    ("own", 0, 1),
    ("line", 0, 0, -1),
    ("line", 0, 0, 1),
    ("own", 1, 0),
    ("line", 0, 1, -1),
    ("own", 1, 1),
    ("target_y",),
    ("onward", 0, 1, 0, 1),
    ("onward", 0, 0, 0, -1),
    ("onward", 0, 0, 0, 1),
    ("line", 1, 0, -1),
    ("line", 0, 1, 1),
    ("onward", 0, 1, 0, -1),
    ("target_z",),
    ("line", 1, 1, 1),
    ("line", 1, 1, -1),
    ("across", 0, 0),
    ("line", 1, 0, 1),
    ("onward", 0, 1, 3, -1),
    ("onward", 0, 0, 1, 1),
    ("onward", 0, 1, 3, 1),
    ("across", 1, 0),
    ("onward", 0, 0, 1, -1),
    ("far", 1, 1),
    ("far", 0, 1),
    ("far", 0, 0),
    ("target_plane",),
    ("far", 1, 0),
    ("onward", 0, 0, 3, -1),
    ("onward", 1, 0, 3, -1),
    ("across", 0, 1),
    ("onward", 1, 1, 1, 1),
    ("onward", 0, 1, 1, -1),
    ("onward", 0, 0, 3, 1),
    ("onward", 1, 1, 2, -1),
    ("onward", 0, 0, 2, -1),
    ("onward", 0, 0, 2, 1),
    ("onward", 0, 1, 1, 1),
    ("onward", 1, 1, 2, 1),
    ("onward", 1, 0, 3, 1),
    ("onward", 1, 1, 1, -1),
    ("across", 1, 3),
    ("onward", 0, 1, 2, 1),
    ("target_core",),
    ("onward", 1, 0, 2, 1),
    ("onward", 1, 0, 2, -1),
    ("onward", 0, 1, 2, -1),
)
ACROSS = tuple(step[1:] for step in ORDER if step[0] == "across")


def nn(left, right):
    return jnp.dot(left, right, preferred_element_type=F32)


def kernel(
    spans,
    states_hbm,
    out_bridge,
    out_residual,
    states,
    keep_x,
    send_x,
    recv_x,
    keep_y,
    send_y,
    recv_y,
    near_x,
    near_y,
    xs,
    y_own,
    y_mid,
    ys,
    yt,
    b_t,
    ab_t,
    parts,
    ar_ship,
    far_b,
    far_ab,
    far_ar,
    low,
    part_out,
    part_in,
    mapped,
    tile_out,
    tile_in,
    sum_y,
    sum_z,
    sum_far,
    send_sems,
    recv_sems,
    load_sem,
):
    load = pltpu.make_async_copy(states_hbm, states, load_sem)
    load.start()
    b = lax.axis_index("xl")
    c = lax.axis_index("core")
    y = lax.axis_index("y")
    z = lax.axis_index("z")
    h = lax.axis_index("xh")
    tokens, width = xs.shape
    scale = 1.0 / tokens
    rows = states.shape[1]
    half = rows // 2
    part = width // 2
    cols = ys.shape[-1]
    side = cols // 2

    def at(xl=b, core=c, yy=y, zz=z, xh=h):
        return (xl, core, yy, zz, xh)

    def step(value, by):
        return lax.rem(value + by, 4)

    sent = []

    class Message:
        def __init__(self, src, dst, device):
            index = len(sent)
            self.copy = pltpu.make_async_remote_copy(
                src_ref=src,
                dst_ref=dst,
                send_sem=send_sems.at[index],
                recv_sem=recv_sems.at[index],
                device_id=device,
                device_id_type=MESH,
            )
            self.copy.start()
            self.arrived = False
            sent.append(self)

        def need(self):
            if not self.arrived:
                self.arrived = True
                self.copy.wait_recv()

    other = at(core=1 - c)
    partner = at(xl=1 - b)
    neighbour = at(xl=1 - b, xh=1 - h)
    opposite = at(xh=1 - h)

    barrier = pltpu.get_barrier_semaphore()
    greeted = [partner, neighbour, opposite, other]
    greeted += [at(yy=step(y, d)) for d in (1, 2, 3)]
    greeted += [at(xl=xl, zz=step(z, d)) for d in (1, 2, 3) for xl in (b, 1 - b)]
    for device in greeted:
        pl.semaphore_signal(barrier, inc=1, device_id=device, device_id_type=MESH)

    load.wait()

    section = 2 * b + c

    def mine(k, which, row, count_rows, column, count_columns):
        there = spans[k, which] - 2 * section
        area = (pl.ds(row, count_rows), pl.ds(column, count_columns))
        first = states[(0, *area)]
        second = states[(1, *area)]
        zero = jnp.zeros_like(first)
        return lax.select_n(there == 0, lax.select_n(there == 1, zero, second), first)

    for k in range(2):
        for block in range(2):
            there = pl.ds(block * part, part)
            here = pl.multiple_of((2 * block + c) * part, part)
            away = pl.multiple_of((2 * block + 1 - c) * part, part)
            send_x[k, :, there] = mine(k, 0, 0, rows, away, part)
            keep_x[k, :, there] = mine(k, 0, 0, rows, here, part)
        send_y[k] = mine(k, 1, pl.multiple_of((1 - c) * half, half), half, 0, 2 * width)
        keep_y[k] = mine(k, 1, pl.multiple_of(c * half, half), half, 0, 2 * width)

    pl.semaphore_wait(barrier, len(greeted))

    quarter = half // 2
    first_rows, later_rows = pl.ds(0, quarter), pl.ds(quarter, rows - quarter)
    pair_far = [
        Message(send_x.at[1 - b, there], recv_x.at[1 - b, there], other)
        for there in (first_rows, later_rows)
    ]
    pair_own = Message(send_x.at[b], recv_x.at[b], other)
    pair_y = Message(send_y, recv_y, other)
    pieces = [pl.ds(piece * half, half) for piece in range(2)]

    quarters = [pl.ds(i * quarter, quarter) for i in range(4)]

    def ring(k, slot, device, parts_of):
        return [
            Message(keep_x.at[k, there], near_x.at[slot, there], device) for there in parts_of
        ]

    from_partner = []
    for copy, there in zip(pair_far, (first_rows, later_rows)):
        copy.need()
        keep_x[1 - b, there] = keep_x[1 - b, there] + recv_x[1 - b, there]
        sent_now = quarters[:1] if there is first_rows else quarters[1:]
        from_partner += ring(1 - b, 0, partner, sent_now)
    from_neighbour = ring(1 - b, 1, neighbour, pieces)
    pair_own.need()
    keep_x[b] = keep_x[b] + recv_x[b]
    pair_y.need()
    keep_y[...] = keep_y[...] + recv_y[...]

    moved = {}

    def place(kind, piece, first, second, sub=None):
        p, q = (first, second) if piece == 0 else (second, first)
        row = (kind * 16 + p * 4 + q) * rows + piece * half
        if sub is None:
            return xs.at[pl.ds(row, half)]
        return xs.at[pl.ds(row + sub * quarter, quarter)]

    def along(piece, leg, by):
        if leg == piece:
            return at(yy=step(y, by % 4))
        return at(zz=step(z, by % 4))

    def spread(kind, piece, first):
        for by in (1, -1):
            moved[kind, piece, first, by] = Message(
                place(kind, piece, first, 0),
                place(kind, piece, first, by % 4),
                along(piece, 1, by),
            )

    class Both:
        def __init__(self, *messages):
            self.messages = messages

        def need(self):
            for message in self.messages:
                message.need()

    def own_part(kind, piece, sub):
        copies = {}
        for leg in (0, 1):
            for by in (1, -1):
                target = (by % 4, 0) if leg == 0 else (0, by % 4)
                copies[leg, by] = Message(
                    place(kind, piece, 0, 0, sub),
                    place(kind, piece, *target, sub),
                    along(piece, leg, by),
                )
        return copies

    def own(kind, piece):
        if kind == 0:
            copies = []
            for sub in range(2):
                there = quarters[2 * piece + sub]
                from_partner[2 * piece + sub].need()
                xs[there, :] = keep_x[b, there, :] + near_x[0, there, :]
                copies.append(own_part(kind, piece, sub))
            copies = {key: Both(copies[0][key], copies[1][key]) for key in copies[0]}
        else:
            here = pieces[piece]
            from_neighbour[piece].need()
            from_opposite[piece].need()
            xs[pl.ds(16 * rows + piece * half, half), :] = near_x[1, here, :] + near_x[2, here, :]
            copies = own_part(kind, piece, None)
        for by in (1, -1):
            moved[kind, piece, "line", by] = copies[0, by]
            moved[kind, piece, 0, by] = copies[1, by]

    def line(kind, piece, by):
        moved[kind, piece, "line", by].need()
        sub = 0 if by == 1 else 1
        moved[kind, piece, "far", by] = Message(
            place(kind, piece, by % 4, 0, sub), place(kind, piece, 2, 0, sub), along(piece, 0, by)
        )
        spread(kind, piece, by % 4)

    def far(kind, piece):
        for by in (1, -1):
            moved[kind, piece, "far", by].need()
        spread(kind, piece, 2)

    def onward(kind, piece, first, by):
        moved[kind, piece, first, by].need()
        sub = 0 if by == 1 else 1
        moved[kind, piece, first, "end", by] = Message(
            place(kind, piece, first, by % 4, sub),
            place(kind, piece, first, 2, sub),
            along(piece, 1, by),
        )

    def across(piece, first):
        for by in (1, -1):
            moved[0, piece, first, "end", by].need()
        moved[1, piece, first, "across"] = Message(
            place(0, piece, first, 2), place(1, piece, first, 2), opposite
        )

    def end(kind, piece, first):
        if kind == 1 and (piece, first) in ACROSS:
            moved[kind, piece, first, "across"].need()
        else:
            for by in (1, -1):
                moved[kind, piece, first, "end", by].need()

    def whole(kind, p):
        for by in (1, -1):
            moved[kind, 0, p, by].need()
        end(kind, 0, p)
        for first in range(4):
            if p == 2:
                end(kind, 1, first)
            elif p:
                moved[kind, 1, first, 1 if p == 1 else -1].need()

    size = 256

    blocks = [pl.ds(j * size, size) for j in range(width // size)]

    def right_part(kind, p, fresh):
        whole(kind, p)
        here = pl.ds((kind * 16 + p * 4) * rows, 4 * rows)
        yt[:, here] = ys[kind, p].reshape(4 * rows, cols).T
        for there in blocks:
            value = nn(yt[:, here], xs[here, there])
            b_t[:, there] = value if fresh else b_t[:, there] + value

    near_target, along_y, along_z, plane, cross = [], [], [], [], []
    from_opposite = []

    def opposite_ring():
        from_opposite.extend(ring(b, 2, opposite, pieces))

    def target():
        near_target.append(Message(keep_y.at[1 - b], near_y, partner))

    def target_y():
        near_target[0].need()
        y_own[...] = keep_y[b] + near_y[...]
        for by in (1, 3, 2):
            to = step(y, by)
            columns = pl.ds(pl.multiple_of(to * 4 * cols, 4 * cols), 4 * cols)
            along_y.append(Message(y_own.at[:, columns], y_mid.at[by], at(yy=to)))
        columns = pl.ds(pl.multiple_of(y * 4 * cols, 4 * cols), 4 * cols)
        y_mid[0] = y_own[:, columns]

    def target_z():
        for copy in along_y:
            copy.need()
        for by in (1, 3, 2):
            to = step(z, by)
            columns = pl.ds(pl.multiple_of(to * cols, cols), cols)
            along_z.append(Message(y_mid.at[:, :, columns], ys.at[0, :, by, c], at(zz=to)))
        columns = pl.ds(pl.multiple_of(z * cols, cols), cols)
        ys[0, :, 0, c] = y_mid[:, :, columns]

    def target_plane():
        for copy in along_z:
            copy.need()
        plane.append(Message(ys.at[0, :, :, c], ys.at[1, :, :, c], opposite))
        cross.append(Message(ys.at[0, :, :, c], ys.at[0, :, :, c], other))

    def target_core():
        plane[0].need()
        cross.append(Message(ys.at[1, :, :, c], ys.at[1, :, :, c], other))

    steps = {
        "own": own,
        "opposite": opposite_ring,
        "line": line,
        "far": far,
        "onward": onward,
        "across": across,
        "target": target,
        "target_y": target_y,
        "target_z": target_z,
        "target_plane": target_plane,
        "target_core": target_core,
    }
    for name, *arguments in ORDER:
        steps[name](*arguments)
    cross[0].need()
    right_part(0, 0, True)
    right_part(0, 1, False)
    right_part(0, 3, False)
    cross[1].need()
    right_part(1, 0, False)
    right_part(1, 1, False)
    right_part(1, 3, False)

    last = []
    for kind in range(2):
        whole(kind, 2)
        here = pl.ds((kind * 16 + 8) * rows, 4 * rows)
        yt[:, here] = ys[kind, 2].reshape(4 * rows, cols).T
        last.append(here)
    zero_row = jnp.zeros((1, size), F32)

    squares = zero_row
    for there in blocks:
        value = b_t[:, there]
        for here in last:
            value = value + nn(yt[:, here], xs[here, there])
        value = value * scale
        b_t[:, there] = value
        low[0, there, :] = value.astype(BF16).T
        squares = squares + jnp.sum(value * value, axis=0, keepdims=True)
    m0 = jnp.sum(squares, axis=1, keepdims=True)
    tile_out[0] = jnp.broadcast_to(m0, (8, 128))
    norm = Message(tile_out.at[0], tile_in.at[0], other)

    shipped = (
        (partner, h * side, (1 - b) * part, 0),
        (neighbour, (1 - h) * side, (1 - b) * part + part // 2, part // 2),
    )

    def ship(source, target):
        return [
            Message(
                source.at[
                    pl.ds(pl.multiple_of(row, side), side),
                    pl.ds(pl.multiple_of(column, part // 2), part // 2),
                ],
                target.at[:, pl.ds(start, part // 2)],
                device,
            )
            for device, row, column, start in shipped
        ]

    arriving = ship(b_t, far_b)

    long = tokens // 4
    token_halves = [pl.ds(i * 2 * long, 2 * long) for i in range(2)]

    def products(turn):
        copies = []
        for part_of in range(4):
            for i in range(long // size):
                value = nn(xs[pl.ds(part_of * long + i * size, size), :], low[turn])
                part_out[turn, part_of, :, pl.ds(i * size, size)] = value.astype(BF16).T
            copies.append(
                Message(part_out.at[turn, part_of], part_in.at[turn, part_of], other)
            )
        return copies

    def add_up(turn, part_of, squares):
        copies[part_of].need()
        for i in range(long // size):
            there = pl.ds(i * size, size)
            value = part_out[turn, part_of, :, there].astype(F32)
            value = value + part_in[turn, part_of, :, there].astype(F32)
            squares = squares + jnp.sum(value * value, axis=0, keepdims=True)
            mapped[:, pl.ds(part_of * long + i * size, size)] = value.astype(BF16)
        return squares

    row = lax.broadcasted_iota(jnp.int32, (8, 128), 0)

    def tile_of(values):
        tile = jnp.zeros((8, 128), F32)
        for i, value in enumerate(values):
            tile = jnp.where(row == i, value, tile)
        return tile

    copies = products(0)
    squares = add_up(0, 1, add_up(0, 0, zero_row))
    for there in blocks:
        ab_t[:, there] = nn(mapped[:, token_halves[0]], xs[token_halves[0], there])
    squares = add_up(0, 3, add_up(0, 2, squares))
    length = jnp.sum(squares, axis=1, keepdims=True) * scale
    norm.need()
    chip_norm = m0 + tile_in[0, 0:1, 0:1]
    chip_curvature = length + RIDGE * chip_norm
    some = chip_curvature > 0.0
    guess = jnp.where(some, chip_norm / jnp.where(some, chip_curvature, 1.0), 1.0)

    sums = [zero_row] * 4
    for there in blocks:
        base = b_t[:, there]
        image = ab_t[:, there] + nn(mapped[:, token_halves[1]], xs[token_halves[1], there])
        image = image * scale + RIDGE * base
        ab_t[:, there] = image
        rest = base - guess * image
        low[1, there, :] = rest.astype(BF16).T
        terms = (base * image, image * image, rest * image, rest * rest)
        sums = [total + jnp.sum(t, axis=0, keepdims=True) for total, t in zip(sums, terms)]
    tile = tile_of([jnp.sum(total, axis=1, keepdims=True) for total in sums])
    tile_out[1] = tile
    pair_sums = Message(tile_out.at[1], tile_in.at[2], other)

    arriving += ship(ab_t, far_ab)
    copies = products(1)
    tile_out[3] = jnp.broadcast_to(guess, (8, 128))
    arriving.append(Message(tile_out.at[3], tile_in.at[1], partner))
    pair_sums.need()
    chip = tile + tile_in[2]
    m1, m2, cross_term, rest_norm = (chip[i : i + 1, 0:1] for i in range(4))
    squares = zero_row
    for part_of in range(4):
        squares = add_up(1, part_of, squares)
    second = jnp.sum(squares, axis=1, keepdims=True) * scale + RIDGE * rest_norm
    m3 = (second - 2.0 * cross_term + m1) / (guess * guess)
    tile = tile_of((chip_norm, m1, m2, m3))
    tile_out[4] = tile
    sum_y[0] = tile
    over_y = [Message(tile_out.at[4], sum_y.at[by], at(yy=step(y, by))) for by in (1, 2, 3)]

    def second_image(side_row, column, count_blocks, put):
        line_rows = pl.ds(pl.multiple_of(side_row, side), side)
        for j in range(count_blocks):
            there = pl.ds(pl.multiple_of(column + j * size, size), size)
            base = b_t[line_rows, there] - guess * ab_t[line_rows, there]
            put(j * size, nn(mapped[line_rows, :], xs[:, there]) * scale + RIDGE * base)

    arriving_rest = []
    for turn, (device, row, column, start) in enumerate(shipped):

        def put(at_column, value):
            ar_ship[turn, :, at_column : at_column + size] = value.astype(BF16)

        second_image(row, column, part // 2 // size, put)
        arriving_rest.append(
            Message(ar_ship.at[turn], far_ar.at[:, pl.ds(start, part // 2)], device)
        )
    for copy in over_y:
        copy.need()
    tile = jnp.sum(sum_y[...], axis=0)
    tile_out[2] = tile
    sum_z[0] = tile
    over_z = [Message(tile_out.at[2], sum_z.at[by], at(zz=step(z, by))) for by in (1, 2, 3)]
    over_z += [
        Message(tile_out.at[2], sum_far.at[by], at(xl=1 - b, zz=step(z, by)))
        for by in (0, 1, 2, 3)
    ]

    line_rows = pl.ds(pl.multiple_of(h * side, side), side)
    there = pl.ds(pl.multiple_of(b * part, part), part)

    def put_own(at_column, value):
        parts[0, 2, pl.ds(at_column, size), :] = value.T

    second_image(h * side, b * part, part // size, put_own)
    parts[0, 0] = b_t[line_rows, there].T
    parts[0, 1] = ab_t[line_rows, there].T
    for copy in arriving:
        copy.need()
    parts[1, 0] = far_b[...].T
    parts[1, 1] = far_ab[...].T

    def finish(k, sums, guess, which):
        m0, m1, m2, m3 = (sums[i : i + 1, 0:1] for i in range(4))
        size1 = m0 / m1
        renewed = m0 - 2.0 * size1 * m1 + size1 * size1 * m2
        ratio = renewed / m0
        more = 1.0 + ratio
        curvature = more * more * m1 - 2.0 * more * size1 * m2 + size1 * size1 * m3
        size2 = renewed / curvature
        of_rest = size1 / guess
        of_base = more - of_rest
        base, image, rest_image = (parts[which, i] for i in range(3))
        out_bridge[k] = (size1 + size2 * more) * base - (size1 * size2) * image
        out_residual[k] = (
            base - (size1 + size2 * of_base) * image - (size2 * of_rest) * rest_image
        )

    for copy in over_z[:3]:
        copy.need()
    finish(b, jnp.sum(sum_z[...], axis=0), guess, 0)
    for copy in arriving_rest:
        copy.need()
    parts[1, 2] = far_ar[...].astype(F32).T
    for copy in over_z[3:]:
        copy.need()
    finish(1 - b, jnp.sum(sum_far[...], axis=0), tile_in[1, 0:1, 0:1], 1)
    for message in sent:
        message.copy.wait_send()


MESSAGES = 168


def per_device(states, spans):
    _, rows, features = states.shape
    tokens = rows * 32
    width = features // 2
    cols = features // 16
    half = rows // 2
    vmem = pltpu.VMEM
    out = jax.ShapeDtypeStruct((2, width // 2, cols // 2), F32)
    return pl.pallas_call(
        kernel,
        out_shape=(out, out),
        in_specs=[
            pl.BlockSpec(memory_space=pltpu.SMEM),
            pl.BlockSpec(memory_space=pltpu.HBM),
        ],
        out_specs=(pl.BlockSpec(memory_space=vmem), pl.BlockSpec(memory_space=vmem)),
        scratch_shapes=[
            vmem((2, rows, features), BF16),
            vmem((2, rows, width), BF16),
            vmem((2, rows, width), BF16),
            vmem((2, rows, width), BF16),
            vmem((2, half, features), BF16),
            vmem((2, half, features), BF16),
            vmem((2, half, features), BF16),
            vmem((3, rows, width), BF16),
            vmem((half, features), BF16),
            vmem((tokens, width), BF16),
            vmem((half, features), BF16),
            vmem((4, half, 4 * cols), BF16),
            vmem((2, 4, 4, 2, half, cols), BF16),
            vmem((cols, tokens), BF16),
            vmem((cols, width), F32),
            vmem((cols, width), F32),
            vmem((2, 3, width // 2, cols // 2), F32),
            vmem((2, cols // 2, width // 4), BF16),
            vmem((cols // 2, width // 2), F32),
            vmem((cols // 2, width // 2), F32),
            vmem((cols // 2, width // 2), BF16),
            vmem((2, width, cols), BF16),
            vmem((2, 4, cols, tokens // 4), BF16),
            vmem((2, 4, cols, tokens // 4), BF16),
            vmem((cols, tokens), BF16),
            vmem((5, 8, 128), F32),
            vmem((3, 8, 128), F32),
            vmem((4, 8, 128), F32),
            vmem((4, 8, 128), F32),
            vmem((4, 8, 128), F32),
            pltpu.SemaphoreType.DMA((MESSAGES,)),
            pltpu.SemaphoreType.DMA((MESSAGES,)),
            pltpu.SemaphoreType.DMA,
        ],
        compiler_params=pltpu.CompilerParams(
            collective_id=0, has_side_effects=True, vmem_limit_bytes=51 * 1024 * 1024
        ),
    )(spans, states)


def solution(mesh):
    split = Mesh(mesh.devices.reshape(2, 2, 4, 4, 2), AXES)
    return jax.shard_map(
        per_device,
        mesh=split,
        in_specs=(P(SECTION, TOK, None), P()),
        out_specs=(P(None, SECTION, TOK), P(None, SECTION, TOK)),
        check_vma=False,
    )
```

```python
import jax
import jax.numpy as jnp
from jax import lax
from jax.experimental import pallas as pl
from jax.experimental.pallas import tpu as pltpu
from jax.sharding import Mesh
from jax.sharding import PartitionSpec as P

MESH = pl.DeviceIdType.MESH
AXES = ("xl", "core", "y", "z", "xh")
SECTION = ("xl", "core")
TOK = ("y", "z", "xh")
RIDGE = 0.25
F32 = jnp.float32
BF16 = jnp.bfloat16


ORDER = (
    ("own", 0, 0),
    ("target",),
    ("own", 0, 1),
    ("onward", 0, 0, 0, -1),
    ("line", 0, 0, -1),
    ("line", 0, 0, 1),
    ("line", 0, 1, -1),
    ("onward", 0, 1, 0, 1),
    ("opposite",),
    ("target_y",),
    ("onward", 0, 0, 3, 1),
    ("onward", 0, 1, 0, -1),
    ("onward", 0, 0, 0, 1),
    ("onward", 0, 0, 3, -1),
    ("line", 0, 1, 1),
    ("own", 1, 0),
    ("own", 1, 1),
    ("across", 0, 0),
    ("across", 0, 3),
    ("onward", 0, 0, 1, 1),
    ("onward", 0, 0, 1, -1),
    ("onward", 0, 1, 3, -1),
    ("across", 1, 0),
    ("onward", 0, 1, 3, 1),
    ("target_z",),
    ("line", 1, 1, -1),
    ("far", 0, 0),
    ("line", 1, 1, 1),
    ("line", 1, 0, 1),
    ("line", 1, 0, -1),
    ("across", 0, 1),
    ("onward", 0, 1, 1, -1),
    ("across", 1, 3),
    ("far", 0, 1),
    ("onward", 0, 1, 1, 1),
    ("far", 1, 1),
    ("target_plane",),
    ("far", 1, 0),
    ("onward", 0, 0, 2, 1),
    ("onward", 0, 1, 2, -1),
    ("across", 1, 1),
    ("onward", 0, 0, 2, -1),
    ("onward", 0, 1, 2, 1),
    ("onward", 1, 0, 2, -1),
    ("onward", 1, 1, 2, -1),
    ("onward", 1, 0, 2, 1),
    ("onward", 1, 1, 2, 1),
    ("target_core",),
)
ACROSS = tuple(step[1:] for step in ORDER if step[0] == "across")


def nn(left, right):
    return jnp.dot(left, right, preferred_element_type=F32)


def kernel(
    spans,
    states_hbm,
    out_bridge,
    out_residual,
    states,
    keep_x,
    send_x,
    recv_x,
    keep_y,
    send_y,
    recv_y,
    near_x,
    near_y,
    xs,
    y_own,
    y_mid,
    ys,
    yt,
    b_t,
    ab_t,
    parts,
    ar_ship,
    far_b,
    far_ab,
    far_ar,
    low,
    part_out,
    part_in,
    mapped,
    tile_out,
    tile_in,
    sum_y,
    sum_z,
    sum_far,
    send_sems,
    recv_sems,
    load_sems,
):
    b = lax.axis_index("xl")
    c = lax.axis_index("core")
    y = lax.axis_index("y")
    z = lax.axis_index("z")
    h = lax.axis_index("xh")
    tokens, width = xs.shape
    scale = 1.0 / tokens
    rows = states.shape[1]
    half = rows // 2
    quarter = half // 2
    first_rows, later_rows = pl.ds(0, quarter), pl.ds(quarter, rows - quarter)
    loads = [
        pltpu.make_async_copy(states_hbm.at[:, there], states.at[:, there], load_sems.at[i])
        for i, there in enumerate((first_rows, later_rows))
    ]
    for load in loads:
        load.start()
    part = width // 2
    cols = ys.shape[-1]
    side = cols // 2

    def at(xl=b, core=c, yy=y, zz=z, xh=h):
        return (xl, core, yy, zz, xh)

    def step(value, by):
        return lax.rem(value + by, 4)

    sent = []

    class Message:
        def __init__(self, src, dst, device):
            index = len(sent)
            self.copy = pltpu.make_async_remote_copy(
                src_ref=src,
                dst_ref=dst,
                send_sem=send_sems.at[index],
                recv_sem=recv_sems.at[index],
                device_id=device,
                device_id_type=MESH,
            )
            self.copy.start()
            self.arrived = False
            sent.append(self)

        def need(self):
            if not self.arrived:
                self.arrived = True
                self.copy.wait_recv()

    other = at(core=1 - c)
    partner = at(xl=1 - b)
    neighbour = at(xl=1 - b, xh=1 - h)
    opposite = at(xh=1 - h)

    barrier = pltpu.get_barrier_semaphore()
    greeted = [partner, neighbour, opposite, other]
    greeted += [at(yy=step(y, d)) for d in (1, 2, 3)]
    greeted += [at(xl=xl, zz=step(z, d)) for d in (1, 2, 3) for xl in (b, 1 - b)]
    for device in greeted:
        pl.semaphore_signal(barrier, inc=1, device_id=device, device_id_type=MESH)

    section = 2 * b + c

    def mine(k, which, row, count_rows, column, count_columns):
        there = spans[k, which] - 2 * section
        area = (pl.ds(row, count_rows), pl.ds(column, count_columns))
        first = states[(0, *area)]
        second = states[(1, *area)]
        zero = jnp.zeros_like(first)
        return lax.select_n(there == 0, lax.select_n(there == 1, zero, second), first)

    def fill(k, row, count_rows):
        for block in range(2):
            area = (k, pl.ds(row, count_rows), pl.ds(block * part, part))
            here = pl.multiple_of((2 * block + c) * part, part)
            away = pl.multiple_of((2 * block + 1 - c) * part, part)
            send_x[area] = mine(k, 0, row, count_rows, away, part)
            keep_x[area] = mine(k, 0, row, count_rows, here, part)

    pieces = [pl.ds(piece * half, half) for piece in range(2)]
    loads[0].wait()
    fill(1 - b, 0, quarter)
    pl.semaphore_wait(barrier, len(greeted))

    pair_far = [Message(send_x.at[1 - b, first_rows], recv_x.at[1 - b, first_rows], other)]
    loads[1].wait()
    fill(1 - b, quarter, rows - quarter)
    pair_far.append(Message(send_x.at[1 - b, later_rows], recv_x.at[1 - b, later_rows], other))
    fill(b, 0, rows)
    pair_own = Message(send_x.at[b], recv_x.at[b], other)
    for k in range(2):
        send_y[k] = mine(k, 1, pl.multiple_of((1 - c) * half, half), half, 0, 2 * width)
        keep_y[k] = mine(k, 1, pl.multiple_of(c * half, half), half, 0, 2 * width)
    pair_y = Message(send_y, recv_y, other)
    quarters = [pl.ds(i * quarter, quarter) for i in range(4)]

    def ring(k, slot, device, parts_of):
        return [
            Message(keep_x.at[k, there], near_x.at[slot, there], device) for there in parts_of
        ]

    from_partner = []
    for copy, there in zip(pair_far, (first_rows, later_rows)):
        copy.need()
        keep_x[1 - b, there] = keep_x[1 - b, there] + recv_x[1 - b, there]
        sent_now = quarters[:1] if there is first_rows else quarters[1:]
        from_partner += ring(1 - b, 0, partner, sent_now)
    from_neighbour = ring(1 - b, 1, neighbour, pieces)
    pair_own.need()
    keep_x[b] = keep_x[b] + recv_x[b]
    pair_y.need()
    keep_y[...] = keep_y[...] + recv_y[...]

    moved = {}

    def place(kind, piece, first, second, sub=None):
        p, q = (first, second) if piece == 0 else (second, first)
        row = (kind * 16 + p * 4 + q) * rows + piece * half
        if sub is None:
            return xs.at[pl.ds(row, half)]
        return xs.at[pl.ds(row + sub * quarter, quarter)]

    def along(piece, leg, by):
        if leg == piece:
            return at(yy=step(y, by % 4))
        return at(zz=step(z, by % 4))

    def spread(kind, piece, first):
        for by in (1, -1):
            moved[kind, piece, first, by] = Message(
                place(kind, piece, first, 0),
                place(kind, piece, first, by % 4),
                along(piece, 1, by),
            )

    class Both:
        def __init__(self, *messages):
            self.messages = messages

        def need(self):
            for message in self.messages:
                message.need()

    def own_part(kind, piece, sub):
        copies = {}
        for leg in (0, 1):
            for by in (1, -1):
                target = (by % 4, 0) if leg == 0 else (0, by % 4)
                copies[leg, by] = Message(
                    place(kind, piece, 0, 0, sub),
                    place(kind, piece, *target, sub),
                    along(piece, leg, by),
                )
        return copies

    def own(kind, piece):
        if kind == 0:
            copies = []
            for sub in range(2):
                there = quarters[2 * piece + sub]
                from_partner[2 * piece + sub].need()
                xs[there, :] = keep_x[b, there, :] + near_x[0, there, :]
                copies.append(own_part(kind, piece, sub))
            copies = {key: Both(copies[0][key], copies[1][key]) for key in copies[0]}
        else:
            here = pieces[piece]
            from_neighbour[piece].need()
            from_opposite[piece].need()
            xs[pl.ds(16 * rows + piece * half, half), :] = near_x[1, here, :] + near_x[2, here, :]
            copies = own_part(kind, piece, None)
        for by in (1, -1):
            moved[kind, piece, "line", by] = copies[0, by]
            moved[kind, piece, 0, by] = copies[1, by]

    def line(kind, piece, by):
        moved[kind, piece, "line", by].need()
        sub = 0 if by == 1 else 1
        moved[kind, piece, "far", by] = Message(
            place(kind, piece, by % 4, 0, sub), place(kind, piece, 2, 0, sub), along(piece, 0, by)
        )
        spread(kind, piece, by % 4)

    def far(kind, piece):
        for by in (1, -1):
            moved[kind, piece, "far", by].need()
        spread(kind, piece, 2)

    def onward(kind, piece, first, by):
        moved[kind, piece, first, by].need()
        sub = 0 if by == 1 else 1
        moved[kind, piece, first, "end", by] = Message(
            place(kind, piece, first, by % 4, sub),
            place(kind, piece, first, 2, sub),
            along(piece, 1, by),
        )

    def across(piece, first):
        for by in (1, -1):
            moved[0, piece, first, "end", by].need()
        moved[1, piece, first, "across"] = Message(
            place(0, piece, first, 2), place(1, piece, first, 2), opposite
        )

    def end(kind, piece, first):
        if kind == 1 and (piece, first) in ACROSS:
            moved[kind, piece, first, "across"].need()
        else:
            for by in (1, -1):
                moved[kind, piece, first, "end", by].need()

    def whole(kind, p):
        for by in (1, -1):
            moved[kind, 0, p, by].need()
        end(kind, 0, p)
        for first in range(4):
            if p == 2:
                end(kind, 1, first)
            elif p:
                moved[kind, 1, first, 1 if p == 1 else -1].need()

    size = 256

    blocks = [pl.ds(j * size, size) for j in range(width // size)]

    def right_part(kind, p, fresh):
        whole(kind, p)
        here = pl.ds((kind * 16 + p * 4) * rows, 4 * rows)
        yt[:, here] = ys[kind, p].reshape(4 * rows, cols).T
        for there in blocks:
            value = nn(yt[:, here], xs[here, there])
            b_t[:, there] = value if fresh else b_t[:, there] + value

    near_target, along_y, along_z, plane, cross = [], [], [], [], []
    from_opposite = []

    def opposite_ring():
        from_opposite.extend(ring(b, 2, opposite, pieces))

    def target():
        near_target.append(Message(keep_y.at[1 - b], near_y, partner))

    def target_y():
        near_target[0].need()
        y_own[...] = keep_y[b] + near_y[...]
        for by in (1, 3, 2):
            to = step(y, by)
            columns = pl.ds(pl.multiple_of(to * 4 * cols, 4 * cols), 4 * cols)
            along_y.append(Message(y_own.at[:, columns], y_mid.at[by], at(yy=to)))
        columns = pl.ds(pl.multiple_of(y * 4 * cols, 4 * cols), 4 * cols)
        y_mid[0] = y_own[:, columns]

    def target_z():
        for copy in along_y:
            copy.need()
        for by in (1, 3, 2):
            to = step(z, by)
            columns = pl.ds(pl.multiple_of(to * cols, cols), cols)
            along_z.append(Message(y_mid.at[:, :, columns], ys.at[0, :, by, c], at(zz=to)))
        columns = pl.ds(pl.multiple_of(z * cols, cols), cols)
        ys[0, :, 0, c] = y_mid[:, :, columns]

    def target_plane():
        for copy in along_z:
            copy.need()
        plane.append(Message(ys.at[0, :, :, c], ys.at[1, :, :, c], opposite))
        cross.append(Message(ys.at[0, :, :, c], ys.at[0, :, :, c], other))

    def target_core():
        plane[0].need()
        cross.append(Message(ys.at[1, :, :, c], ys.at[1, :, :, c], other))

    steps = {
        "own": own,
        "opposite": opposite_ring,
        "line": line,
        "far": far,
        "onward": onward,
        "across": across,
        "target": target,
        "target_y": target_y,
        "target_z": target_z,
        "target_plane": target_plane,
        "target_core": target_core,
    }
    for name, *arguments in ORDER:
        steps[name](*arguments)
    cross[0].need()
    right_part(0, 0, True)
    right_part(0, 1, False)
    right_part(0, 3, False)
    cross[1].need()
    right_part(1, 0, False)
    right_part(1, 1, False)
    right_part(1, 3, False)

    last = []
    for kind in range(2):
        whole(kind, 2)
        here = pl.ds((kind * 16 + 8) * rows, 4 * rows)
        yt[:, here] = ys[kind, 2].reshape(4 * rows, cols).T
        last.append(here)
    zero_row = jnp.zeros((1, size), F32)

    squares = zero_row
    for there in blocks:
        value = b_t[:, there]
        for here in last:
            value = value + nn(yt[:, here], xs[here, there])
        value = value * scale
        b_t[:, there] = value
        low[0, there, :] = value.astype(BF16).T
        squares = squares + jnp.sum(value * value, axis=0, keepdims=True)
    m0 = jnp.sum(squares, axis=1, keepdims=True)
    tile_out[0] = jnp.broadcast_to(m0, (8, 128))
    norm = Message(tile_out.at[0], tile_in.at[0], other)

    shipped = (
        (partner, h * side, (1 - b) * part, 0),
        (neighbour, (1 - h) * side, (1 - b) * part + part // 2, part // 2),
    )

    def ship(source, target):
        return [
            Message(
                source.at[
                    pl.ds(pl.multiple_of(row, side), side),
                    pl.ds(pl.multiple_of(column, part // 2), part // 2),
                ],
                target.at[:, pl.ds(start, part // 2)],
                device,
            )
            for device, row, column, start in shipped
        ]

    arriving = ship(b_t, far_b)

    long = tokens // 4
    token_halves = [pl.ds(i * 2 * long, 2 * long) for i in range(2)]

    def products(turn):
        copies = []
        for part_of in range(4):
            for i in range(long // size):
                value = nn(xs[pl.ds(part_of * long + i * size, size), :], low[turn])
                part_out[turn, part_of, :, pl.ds(i * size, size)] = value.astype(BF16).T
            copies.append(
                Message(part_out.at[turn, part_of], part_in.at[turn, part_of], other)
            )
        return copies

    def add_up(turn, part_of, squares):
        copies[part_of].need()
        for i in range(long // size):
            there = pl.ds(i * size, size)
            value = part_out[turn, part_of, :, there].astype(F32)
            value = value + part_in[turn, part_of, :, there].astype(F32)
            squares = squares + jnp.sum(value * value, axis=0, keepdims=True)
            mapped[:, pl.ds(part_of * long + i * size, size)] = value.astype(BF16)
        return squares

    row = lax.broadcasted_iota(jnp.int32, (8, 128), 0)

    def tile_of(values):
        tile = jnp.zeros((8, 128), F32)
        for i, value in enumerate(values):
            tile = jnp.where(row == i, value, tile)
        return tile

    copies = products(0)
    squares = add_up(0, 1, add_up(0, 0, zero_row))
    for there in blocks:
        ab_t[:, there] = nn(mapped[:, token_halves[0]], xs[token_halves[0], there])
    squares = add_up(0, 3, add_up(0, 2, squares))
    length = jnp.sum(squares, axis=1, keepdims=True) * scale
    norm.need()
    chip_norm = m0 + tile_in[0, 0:1, 0:1]
    chip_curvature = length + RIDGE * chip_norm
    some = chip_curvature > 0.0
    guess = jnp.where(some, chip_norm / jnp.where(some, chip_curvature, 1.0), 1.0)

    sums = [zero_row] * 4
    for there in blocks:
        base = b_t[:, there]
        image = ab_t[:, there] + nn(mapped[:, token_halves[1]], xs[token_halves[1], there])
        image = image * scale + RIDGE * base
        ab_t[:, there] = image
        rest = base - guess * image
        low[1, there, :] = rest.astype(BF16).T
        terms = (base * image, image * image, rest * image, rest * rest)
        sums = [total + jnp.sum(t, axis=0, keepdims=True) for total, t in zip(sums, terms)]
    tile = tile_of([jnp.sum(total, axis=1, keepdims=True) for total in sums])
    tile_out[1] = tile
    pair_sums = Message(tile_out.at[1], tile_in.at[2], other)

    arriving += ship(ab_t, far_ab)
    copies = products(1)
    tile_out[3] = jnp.broadcast_to(guess, (8, 128))
    arriving.append(Message(tile_out.at[3], tile_in.at[1], partner))
    pair_sums.need()
    chip = tile + tile_in[2]
    m1, m2, cross_term, rest_norm = (chip[i : i + 1, 0:1] for i in range(4))
    squares = zero_row
    for part_of in range(4):
        squares = add_up(1, part_of, squares)
    second = jnp.sum(squares, axis=1, keepdims=True) * scale + RIDGE * rest_norm
    m3 = (second - 2.0 * cross_term + m1) / (guess * guess)
    tile = tile_of((chip_norm, m1, m2, m3))
    tile_out[4] = tile
    sum_y[0] = tile
    over_y = [Message(tile_out.at[4], sum_y.at[by], at(yy=step(y, by))) for by in (1, 2, 3)]

    def second_image(side_row, column, count_blocks, put):
        line_rows = pl.ds(pl.multiple_of(side_row, side), side)
        for j in range(count_blocks):
            there = pl.ds(pl.multiple_of(column + j * size, size), size)
            base = b_t[line_rows, there] - guess * ab_t[line_rows, there]
            put(j * size, nn(mapped[line_rows, :], xs[:, there]) * scale + RIDGE * base)

    arriving_rest = []
    for turn, (device, row, column, start) in enumerate(shipped):

        def put(at_column, value):
            ar_ship[turn, :, at_column : at_column + size] = value.astype(BF16)

        second_image(row, column, part // 2 // size, put)
        arriving_rest.append(
            Message(ar_ship.at[turn], far_ar.at[:, pl.ds(start, part // 2)], device)
        )
    for copy in over_y:
        copy.need()
    tile = jnp.sum(sum_y[...], axis=0)
    tile_out[2] = tile
    sum_z[0] = tile
    over_z = [Message(tile_out.at[2], sum_z.at[by], at(zz=step(z, by))) for by in (1, 2, 3)]
    over_z += [
        Message(tile_out.at[2], sum_far.at[by], at(xl=1 - b, zz=step(z, by)))
        for by in (0, 1, 2, 3)
    ]

    line_rows = pl.ds(pl.multiple_of(h * side, side), side)
    there = pl.ds(pl.multiple_of(b * part, part), part)

    def put_own(at_column, value):
        parts[0, 2, pl.ds(at_column, size), :] = value.T

    second_image(h * side, b * part, part // size, put_own)
    parts[0, 0] = b_t[line_rows, there].T
    parts[0, 1] = ab_t[line_rows, there].T
    for copy in arriving:
        copy.need()
    parts[1, 0] = far_b[...].T
    parts[1, 1] = far_ab[...].T

    def finish(k, sums, guess, which):
        m0, m1, m2, m3 = (sums[i : i + 1, 0:1] for i in range(4))
        size1 = m0 / m1
        renewed = m0 - 2.0 * size1 * m1 + size1 * size1 * m2
        ratio = renewed / m0
        more = 1.0 + ratio
        curvature = more * more * m1 - 2.0 * more * size1 * m2 + size1 * size1 * m3
        size2 = renewed / curvature
        of_rest = size1 / guess
        of_base = more - of_rest
        base, image, rest_image = (parts[which, i] for i in range(3))
        out_bridge[k] = (size1 + size2 * more) * base - (size1 * size2) * image
        out_residual[k] = (
            base - (size1 + size2 * of_base) * image - (size2 * of_rest) * rest_image
        )

    for copy in over_z[:3]:
        copy.need()
    finish(b, jnp.sum(sum_z[...], axis=0), guess, 0)
    for copy in arriving_rest:
        copy.need()
    parts[1, 2] = far_ar[...].astype(F32).T
    for copy in over_z[3:]:
        copy.need()
    finish(1 - b, jnp.sum(sum_far[...], axis=0), tile_in[1, 0:1, 0:1], 1)
    for message in sent:
        message.copy.wait_send()


MESSAGES = 168


def per_device(states, spans):
    _, rows, features = states.shape
    tokens = rows * 32
    width = features // 2
    cols = features // 16
    half = rows // 2
    vmem = pltpu.VMEM
    out = jax.ShapeDtypeStruct((2, width // 2, cols // 2), F32)
    return pl.pallas_call(
        kernel,
        out_shape=(out, out),
        in_specs=[
            pl.BlockSpec(memory_space=pltpu.SMEM),
            pl.BlockSpec(memory_space=pltpu.HBM),
        ],
        out_specs=(pl.BlockSpec(memory_space=vmem), pl.BlockSpec(memory_space=vmem)),
        scratch_shapes=[
            vmem((2, rows, features), BF16),
            vmem((2, rows, width), BF16),
            vmem((2, rows, width), BF16),
            vmem((2, rows, width), BF16),
            vmem((2, half, features), BF16),
            vmem((2, half, features), BF16),
            vmem((2, half, features), BF16),
            vmem((3, rows, width), BF16),
            vmem((half, features), BF16),
            vmem((tokens, width), BF16),
            vmem((half, features), BF16),
            vmem((4, half, 4 * cols), BF16),
            vmem((2, 4, 4, 2, half, cols), BF16),
            vmem((cols, tokens), BF16),
            vmem((cols, width), F32),
            vmem((cols, width), F32),
            vmem((2, 3, width // 2, cols // 2), F32),
            vmem((2, cols // 2, width // 4), BF16),
            vmem((cols // 2, width // 2), F32),
            vmem((cols // 2, width // 2), F32),
            vmem((cols // 2, width // 2), BF16),
            vmem((2, width, cols), BF16),
            vmem((2, 4, cols, tokens // 4), BF16),
            vmem((2, 4, cols, tokens // 4), BF16),
            vmem((cols, tokens), BF16),
            vmem((5, 8, 128), F32),
            vmem((3, 8, 128), F32),
            vmem((4, 8, 128), F32),
            vmem((4, 8, 128), F32),
            vmem((4, 8, 128), F32),
            pltpu.SemaphoreType.DMA((MESSAGES,)),
            pltpu.SemaphoreType.DMA((MESSAGES,)),
            pltpu.SemaphoreType.DMA((2,)),
        ],
        compiler_params=pltpu.CompilerParams(
            collective_id=0, has_side_effects=True, vmem_limit_bytes=51 * 1024 * 1024
        ),
    )(spans, states)


def solution(mesh):
    split = Mesh(mesh.devices.reshape(2, 2, 4, 4, 2), AXES)
    return jax.shard_map(
        per_device,
        mesh=split,
        in_specs=(P(SECTION, TOK, None), P()),
        out_specs=(P(None, SECTION, TOK), P(None, SECTION, TOK)),
        check_vma=False,
    )
```

```python
import jax
import jax.numpy as jnp
from jax import lax
from jax.experimental import pallas as pl
from jax.experimental.pallas import tpu as pltpu
from jax.sharding import Mesh
from jax.sharding import PartitionSpec as P

MESH = pl.DeviceIdType.MESH
AXES = ("xl", "core", "y", "z", "xh")
SECTION = ("xl", "core")
TOK = ("y", "z", "xh")
RIDGE = 0.25
F32 = jnp.float32
BF16 = jnp.bfloat16


ORDER = (
    ("own", 0, 0),
    ("target",),
    ("own", 0, 1),
    ("onward", 0, 0, 0, -1),
    ("line", 0, 0, -1),
    ("line", 0, 0, 1),
    ("line", 0, 1, -1),
    ("onward", 0, 1, 0, 1),
    ("opposite",),
    ("target_y",),
    ("onward", 0, 0, 3, 1),
    ("onward", 0, 1, 0, -1),
    ("onward", 0, 0, 0, 1),
    ("onward", 0, 0, 3, -1),
    ("line", 0, 1, 1),
    ("own", 1, 0),
    ("own", 1, 1),
    ("across", 0, 0),
    ("across", 0, 3),
    ("onward", 0, 0, 1, 1),
    ("onward", 0, 0, 1, -1),
    ("onward", 0, 1, 3, -1),
    ("across", 1, 0),
    ("onward", 0, 1, 3, 1),
    ("target_z",),
    ("line", 1, 1, -1),
    ("far", 0, 0),
    ("line", 1, 1, 1),
    ("line", 1, 0, 1),
    ("line", 1, 0, -1),
    ("across", 0, 1),
    ("onward", 0, 1, 1, -1),
    ("across", 1, 3),
    ("far", 0, 1),
    ("onward", 0, 1, 1, 1),
    ("far", 1, 1),
    ("target_plane",),
    ("far", 1, 0),
    ("onward", 0, 0, 2, 1),
    ("right", 0, 0, True),
    ("onward", 0, 1, 2, -1),
    ("across", 1, 1),
    ("onward", 0, 0, 2, -1),
    ("onward", 0, 1, 2, 1),
    ("right", 0, 1, False),
    ("right", 0, 3, False),
    ("onward", 1, 0, 2, -1),
    ("onward", 1, 1, 2, -1),
    ("onward", 1, 0, 2, 1),
    ("onward", 1, 1, 2, 1),
    ("target_core",),
)
ACROSS = tuple(step[1:] for step in ORDER if step[0] == "across")


def nn(left, right):
    return jnp.dot(left, right, preferred_element_type=F32)


def kernel(
    spans,
    states_hbm,
    out_bridge,
    out_residual,
    states,
    keep_x,
    send_x,
    recv_x,
    keep_y,
    send_y,
    recv_y,
    near_x,
    near_y,
    xs,
    y_own,
    y_mid,
    ys,
    yt,
    b_t,
    ab_t,
    parts,
    ar_ship,
    far_b,
    far_ab,
    far_ar,
    low,
    part_out,
    part_in,
    mapped,
    tile_out,
    tile_in,
    sum_y,
    sum_z,
    sum_far,
    send_sems,
    recv_sems,
    load_sems,
):
    b = lax.axis_index("xl")
    c = lax.axis_index("core")
    y = lax.axis_index("y")
    z = lax.axis_index("z")
    h = lax.axis_index("xh")
    tokens, width = xs.shape
    scale = 1.0 / tokens
    rows = states.shape[1]
    half = rows // 2
    quarter = half // 2
    first_rows, later_rows = pl.ds(0, quarter), pl.ds(quarter, rows - quarter)
    loads = [
        pltpu.make_async_copy(states_hbm.at[:, there], states.at[:, there], load_sems.at[i])
        for i, there in enumerate((first_rows, later_rows))
    ]
    for load in loads:
        load.start()
    part = width // 2
    cols = ys.shape[-1]
    side = cols // 2

    def at(xl=b, core=c, yy=y, zz=z, xh=h):
        return (xl, core, yy, zz, xh)

    def step(value, by):
        return lax.rem(value + by, 4)

    sent = []

    class Message:
        def __init__(self, src, dst, device):
            index = len(sent)
            self.copy = pltpu.make_async_remote_copy(
                src_ref=src,
                dst_ref=dst,
                send_sem=send_sems.at[index],
                recv_sem=recv_sems.at[index],
                device_id=device,
                device_id_type=MESH,
            )
            self.copy.start()
            self.arrived = False
            sent.append(self)

        def need(self):
            if not self.arrived:
                self.arrived = True
                self.copy.wait_recv()

    other = at(core=1 - c)
    partner = at(xl=1 - b)
    neighbour = at(xl=1 - b, xh=1 - h)
    opposite = at(xh=1 - h)

    barrier = pltpu.get_barrier_semaphore()
    greeted = [partner, neighbour, opposite, other]
    greeted += [at(yy=step(y, d)) for d in (1, 2, 3)]
    greeted += [at(xl=xl, zz=step(z, d)) for d in (1, 2, 3) for xl in (b, 1 - b)]
    for device in greeted:
        pl.semaphore_signal(barrier, inc=1, device_id=device, device_id_type=MESH)

    section = 2 * b + c

    def mine(k, which, row, count_rows, column, count_columns):
        there = spans[k, which] - 2 * section
        area = (pl.ds(row, count_rows), pl.ds(column, count_columns))
        first = states[(0, *area)]
        second = states[(1, *area)]
        zero = jnp.zeros_like(first)
        return lax.select_n(there == 0, lax.select_n(there == 1, zero, second), first)

    def fill(k, row, count_rows):
        for block in range(2):
            area = (k, pl.ds(row, count_rows), pl.ds(block * part, part))
            here = pl.multiple_of((2 * block + c) * part, part)
            away = pl.multiple_of((2 * block + 1 - c) * part, part)
            send_x[area] = mine(k, 0, row, count_rows, away, part)
            keep_x[area] = mine(k, 0, row, count_rows, here, part)

    pieces = [pl.ds(piece * half, half) for piece in range(2)]
    loads[0].wait()
    fill(1 - b, 0, quarter)
    pl.semaphore_wait(barrier, len(greeted))

    pair_far = [Message(send_x.at[1 - b, first_rows], recv_x.at[1 - b, first_rows], other)]
    loads[1].wait()
    fill(1 - b, quarter, rows - quarter)
    pair_far.append(Message(send_x.at[1 - b, later_rows], recv_x.at[1 - b, later_rows], other))
    fill(b, 0, rows)
    pair_own = Message(send_x.at[b], recv_x.at[b], other)
    for k in range(2):
        send_y[k] = mine(k, 1, pl.multiple_of((1 - c) * half, half), half, 0, 2 * width)
        keep_y[k] = mine(k, 1, pl.multiple_of(c * half, half), half, 0, 2 * width)
    pair_y = Message(send_y, recv_y, other)
    quarters = [pl.ds(i * quarter, quarter) for i in range(4)]

    def ring(k, slot, device, parts_of):
        return [
            Message(keep_x.at[k, there], near_x.at[slot, there], device) for there in parts_of
        ]

    from_partner = []
    for copy, there in zip(pair_far, (first_rows, later_rows)):
        copy.need()
        keep_x[1 - b, there] = keep_x[1 - b, there] + recv_x[1 - b, there]
        sent_now = quarters[:1] if there is first_rows else quarters[1:]
        from_partner += ring(1 - b, 0, partner, sent_now)
    from_neighbour = ring(1 - b, 1, neighbour, pieces)
    pair_own.need()
    keep_x[b] = keep_x[b] + recv_x[b]
    pair_y.need()
    keep_y[...] = keep_y[...] + recv_y[...]

    moved = {}

    def place(kind, piece, first, second, sub=None):
        p, q = (first, second) if piece == 0 else (second, first)
        row = (kind * 16 + p * 4 + q) * rows + piece * half
        if sub is None:
            return xs.at[pl.ds(row, half)]
        return xs.at[pl.ds(row + sub * quarter, quarter)]

    def along(piece, leg, by):
        if leg == piece:
            return at(yy=step(y, by % 4))
        return at(zz=step(z, by % 4))

    def spread(kind, piece, first):
        for by in (1, -1):
            moved[kind, piece, first, by] = Message(
                place(kind, piece, first, 0),
                place(kind, piece, first, by % 4),
                along(piece, 1, by),
            )

    class Both:
        def __init__(self, *messages):
            self.messages = messages

        def need(self):
            for message in self.messages:
                message.need()

    def own_part(kind, piece, sub):
        copies = {}
        for leg in (0, 1):
            for by in (1, -1):
                target = (by % 4, 0) if leg == 0 else (0, by % 4)
                copies[leg, by] = Message(
                    place(kind, piece, 0, 0, sub),
                    place(kind, piece, *target, sub),
                    along(piece, leg, by),
                )
        return copies

    def own(kind, piece):
        if kind == 0:
            copies = []
            for sub in range(2):
                there = quarters[2 * piece + sub]
                from_partner[2 * piece + sub].need()
                xs[there, :] = keep_x[b, there, :] + near_x[0, there, :]
                copies.append(own_part(kind, piece, sub))
            copies = {key: Both(copies[0][key], copies[1][key]) for key in copies[0]}
        else:
            here = pieces[piece]
            from_neighbour[piece].need()
            from_opposite[piece].need()
            xs[pl.ds(16 * rows + piece * half, half), :] = near_x[1, here, :] + near_x[2, here, :]
            copies = own_part(kind, piece, None)
        for by in (1, -1):
            moved[kind, piece, "line", by] = copies[0, by]
            moved[kind, piece, 0, by] = copies[1, by]

    def line(kind, piece, by):
        moved[kind, piece, "line", by].need()
        sub = 0 if by == 1 else 1
        moved[kind, piece, "far", by] = Message(
            place(kind, piece, by % 4, 0, sub), place(kind, piece, 2, 0, sub), along(piece, 0, by)
        )
        spread(kind, piece, by % 4)

    def far(kind, piece):
        for by in (1, -1):
            moved[kind, piece, "far", by].need()
        spread(kind, piece, 2)

    def onward(kind, piece, first, by):
        moved[kind, piece, first, by].need()
        sub = 0 if by == 1 else 1
        moved[kind, piece, first, "end", by] = Message(
            place(kind, piece, first, by % 4, sub),
            place(kind, piece, first, 2, sub),
            along(piece, 1, by),
        )

    def across(piece, first):
        for by in (1, -1):
            moved[0, piece, first, "end", by].need()
        moved[1, piece, first, "across"] = Message(
            place(0, piece, first, 2), place(1, piece, first, 2), opposite
        )

    def end(kind, piece, first):
        if kind == 1 and (piece, first) in ACROSS:
            moved[kind, piece, first, "across"].need()
        else:
            for by in (1, -1):
                moved[kind, piece, first, "end", by].need()

    def whole(kind, p):
        for by in (1, -1):
            moved[kind, 0, p, by].need()
        end(kind, 0, p)
        for first in range(4):
            if p == 2:
                end(kind, 1, first)
            elif p:
                moved[kind, 1, first, 1 if p == 1 else -1].need()

    size = 256

    blocks = [pl.ds(j * size, size) for j in range(width // size)]

    def right_part(kind, p, fresh):
        cross[kind].need()
        whole(kind, p)
        here = pl.ds((kind * 16 + p * 4) * rows, 4 * rows)
        yt[:, here] = ys[kind, p].reshape(4 * rows, cols).T
        for there in blocks:
            value = nn(yt[:, here], xs[here, there])
            b_t[:, there] = value if fresh else b_t[:, there] + value

    near_target, along_y, along_z, plane, cross = [], [], [], [], []
    from_opposite = []

    def opposite_ring():
        from_opposite.extend(ring(b, 2, opposite, pieces))

    def target():
        near_target.append(Message(keep_y.at[1 - b], near_y, partner))

    def target_y():
        near_target[0].need()
        y_own[...] = keep_y[b] + near_y[...]
        for by in (1, 3, 2):
            to = step(y, by)
            columns = pl.ds(pl.multiple_of(to * 4 * cols, 4 * cols), 4 * cols)
            along_y.append(Message(y_own.at[:, columns], y_mid.at[by], at(yy=to)))
        columns = pl.ds(pl.multiple_of(y * 4 * cols, 4 * cols), 4 * cols)
        y_mid[0] = y_own[:, columns]

    def target_z():
        for copy in along_y:
            copy.need()
        for by in (1, 3, 2):
            to = step(z, by)
            columns = pl.ds(pl.multiple_of(to * cols, cols), cols)
            along_z.append(Message(y_mid.at[:, :, columns], ys.at[0, :, by, c], at(zz=to)))
        columns = pl.ds(pl.multiple_of(z * cols, cols), cols)
        ys[0, :, 0, c] = y_mid[:, :, columns]

    def target_plane():
        for copy in along_z:
            copy.need()
        plane.append(Message(ys.at[0, :, :, c], ys.at[1, :, :, c], opposite))
        cross.append(Message(ys.at[0, :, :, c], ys.at[0, :, :, c], other))

    def target_core():
        plane[0].need()
        cross.append(Message(ys.at[1, :, :, c], ys.at[1, :, :, c], other))

    steps = {
        "own": own,
        "opposite": opposite_ring,
        "line": line,
        "far": far,
        "onward": onward,
        "across": across,
        "target": target,
        "target_y": target_y,
        "target_z": target_z,
        "target_plane": target_plane,
        "target_core": target_core,
        "right": right_part,
    }
    for name, *arguments in ORDER:
        steps[name](*arguments)
    right_part(1, 0, False)
    right_part(1, 1, False)
    right_part(1, 3, False)

    last = []
    for kind in range(2):
        whole(kind, 2)
        here = pl.ds((kind * 16 + 8) * rows, 4 * rows)
        yt[:, here] = ys[kind, 2].reshape(4 * rows, cols).T
        last.append(here)
    zero_row = jnp.zeros((1, size), F32)

    squares = zero_row
    for there in blocks:
        value = b_t[:, there]
        for here in last:
            value = value + nn(yt[:, here], xs[here, there])
        value = value * scale
        b_t[:, there] = value
        low[0, there, :] = value.astype(BF16).T
        squares = squares + jnp.sum(value * value, axis=0, keepdims=True)
    m0 = jnp.sum(squares, axis=1, keepdims=True)
    tile_out[0] = jnp.broadcast_to(m0, (8, 128))
    norm = Message(tile_out.at[0], tile_in.at[0], other)

    shipped = (
        (partner, h * side, (1 - b) * part, 0),
        (neighbour, (1 - h) * side, (1 - b) * part + part // 2, part // 2),
    )

    def ship(source, target):
        return [
            Message(
                source.at[
                    pl.ds(pl.multiple_of(row, side), side),
                    pl.ds(pl.multiple_of(column, part // 2), part // 2),
                ],
                target.at[:, pl.ds(start, part // 2)],
                device,
            )
            for device, row, column, start in shipped
        ]

    arriving = ship(b_t, far_b)

    long = tokens // 4
    token_halves = [pl.ds(i * 2 * long, 2 * long) for i in range(2)]

    def products(turn):
        copies = []
        for part_of in range(4):
            for i in range(long // size):
                value = nn(xs[pl.ds(part_of * long + i * size, size), :], low[turn])
                part_out[turn, part_of, :, pl.ds(i * size, size)] = value.astype(BF16).T
            copies.append(
                Message(part_out.at[turn, part_of], part_in.at[turn, part_of], other)
            )
        return copies

    def add_up(turn, part_of, squares):
        copies[part_of].need()
        for i in range(long // size):
            there = pl.ds(i * size, size)
            value = part_out[turn, part_of, :, there].astype(F32)
            value = value + part_in[turn, part_of, :, there].astype(F32)
            squares = squares + jnp.sum(value * value, axis=0, keepdims=True)
            mapped[:, pl.ds(part_of * long + i * size, size)] = value.astype(BF16)
        return squares

    row = lax.broadcasted_iota(jnp.int32, (8, 128), 0)

    def tile_of(values):
        tile = jnp.zeros((8, 128), F32)
        for i, value in enumerate(values):
            tile = jnp.where(row == i, value, tile)
        return tile

    copies = products(0)
    squares = add_up(0, 1, add_up(0, 0, zero_row))
    for there in blocks:
        ab_t[:, there] = nn(mapped[:, token_halves[0]], xs[token_halves[0], there])
    squares = add_up(0, 3, add_up(0, 2, squares))
    length = jnp.sum(squares, axis=1, keepdims=True) * scale
    norm.need()
    chip_norm = m0 + tile_in[0, 0:1, 0:1]
    chip_curvature = length + RIDGE * chip_norm
    some = chip_curvature > 0.0
    guess = jnp.where(some, chip_norm / jnp.where(some, chip_curvature, 1.0), 1.0)

    sums = [zero_row] * 4
    for there in blocks:
        base = b_t[:, there]
        image = ab_t[:, there] + nn(mapped[:, token_halves[1]], xs[token_halves[1], there])
        image = image * scale + RIDGE * base
        ab_t[:, there] = image
        rest = base - guess * image
        low[1, there, :] = rest.astype(BF16).T
        terms = (base * image, image * image, rest * image, rest * rest)
        sums = [total + jnp.sum(t, axis=0, keepdims=True) for total, t in zip(sums, terms)]
    tile = tile_of([jnp.sum(total, axis=1, keepdims=True) for total in sums])
    tile_out[1] = tile
    pair_sums = Message(tile_out.at[1], tile_in.at[2], other)

    arriving += ship(ab_t, far_ab)
    copies = products(1)
    tile_out[3] = jnp.broadcast_to(guess, (8, 128))
    arriving.append(Message(tile_out.at[3], tile_in.at[1], partner))
    pair_sums.need()
    chip = tile + tile_in[2]
    m1, m2, cross_term, rest_norm = (chip[i : i + 1, 0:1] for i in range(4))
    squares = zero_row
    for part_of in range(4):
        squares = add_up(1, part_of, squares)
    second = jnp.sum(squares, axis=1, keepdims=True) * scale + RIDGE * rest_norm
    m3 = (second - 2.0 * cross_term + m1) / (guess * guess)
    tile = tile_of((chip_norm, m1, m2, m3))
    tile_out[4] = tile
    sum_y[0] = tile
    over_y = [Message(tile_out.at[4], sum_y.at[by], at(yy=step(y, by))) for by in (1, 2, 3)]

    def second_image(side_row, column, count_blocks, put):
        line_rows = pl.ds(pl.multiple_of(side_row, side), side)
        for j in range(count_blocks):
            there = pl.ds(pl.multiple_of(column + j * size, size), size)
            base = b_t[line_rows, there] - guess * ab_t[line_rows, there]
            put(j * size, nn(mapped[line_rows, :], xs[:, there]) * scale + RIDGE * base)

    arriving_rest = []
    for turn, (device, row, column, start) in enumerate(shipped):

        def put(at_column, value):
            ar_ship[turn, :, at_column : at_column + size] = value.astype(BF16)

        second_image(row, column, part // 2 // size, put)
        arriving_rest.append(
            Message(ar_ship.at[turn], far_ar.at[:, pl.ds(start, part // 2)], device)
        )
    for copy in over_y:
        copy.need()
    tile = jnp.sum(sum_y[...], axis=0)
    tile_out[2] = tile
    sum_z[0] = tile
    over_z = [Message(tile_out.at[2], sum_z.at[by], at(zz=step(z, by))) for by in (1, 2, 3)]
    over_z += [
        Message(tile_out.at[2], sum_far.at[by], at(xl=1 - b, zz=step(z, by)))
        for by in (0, 1, 2, 3)
    ]

    line_rows = pl.ds(pl.multiple_of(h * side, side), side)
    there = pl.ds(pl.multiple_of(b * part, part), part)

    def put_own(at_column, value):
        parts[0, 2, pl.ds(at_column, size), :] = value.T

    second_image(h * side, b * part, part // size, put_own)
    parts[0, 0] = b_t[line_rows, there].T
    parts[0, 1] = ab_t[line_rows, there].T
    for copy in arriving:
        copy.need()
    parts[1, 0] = far_b[...].T
    parts[1, 1] = far_ab[...].T

    def finish(k, sums, guess, which):
        m0, m1, m2, m3 = (sums[i : i + 1, 0:1] for i in range(4))
        size1 = m0 / m1
        renewed = m0 - 2.0 * size1 * m1 + size1 * size1 * m2
        ratio = renewed / m0
        more = 1.0 + ratio
        curvature = more * more * m1 - 2.0 * more * size1 * m2 + size1 * size1 * m3
        size2 = renewed / curvature
        of_rest = size1 / guess
        of_base = more - of_rest
        base, image, rest_image = (parts[which, i] for i in range(3))
        out_bridge[k] = (size1 + size2 * more) * base - (size1 * size2) * image
        out_residual[k] = (
            base - (size1 + size2 * of_base) * image - (size2 * of_rest) * rest_image
        )

    for copy in over_z[:3]:
        copy.need()
    finish(b, jnp.sum(sum_z[...], axis=0), guess, 0)
    for copy in arriving_rest:
        copy.need()
    parts[1, 2] = far_ar[...].astype(F32).T
    for copy in over_z[3:]:
        copy.need()
    finish(1 - b, jnp.sum(sum_far[...], axis=0), tile_in[1, 0:1, 0:1], 1)
    for message in sent:
        message.copy.wait_send()


MESSAGES = 168


def per_device(states, spans):
    _, rows, features = states.shape
    tokens = rows * 32
    width = features // 2
    cols = features // 16
    half = rows // 2
    vmem = pltpu.VMEM
    out = jax.ShapeDtypeStruct((2, width // 2, cols // 2), F32)
    return pl.pallas_call(
        kernel,
        out_shape=(out, out),
        in_specs=[
            pl.BlockSpec(memory_space=pltpu.SMEM),
            pl.BlockSpec(memory_space=pltpu.HBM),
        ],
        out_specs=(pl.BlockSpec(memory_space=vmem), pl.BlockSpec(memory_space=vmem)),
        scratch_shapes=[
            vmem((2, rows, features), BF16),
            vmem((2, rows, width), BF16),
            vmem((2, rows, width), BF16),
            vmem((2, rows, width), BF16),
            vmem((2, half, features), BF16),
            vmem((2, half, features), BF16),
            vmem((2, half, features), BF16),
            vmem((3, rows, width), BF16),
            vmem((half, features), BF16),
            vmem((tokens, width), BF16),
            vmem((half, features), BF16),
            vmem((4, half, 4 * cols), BF16),
            vmem((2, 4, 4, 2, half, cols), BF16),
            vmem((cols, tokens), BF16),
            vmem((cols, width), F32),
            vmem((cols, width), F32),
            vmem((2, 3, width // 2, cols // 2), F32),
            vmem((2, cols // 2, width // 4), BF16),
            vmem((cols // 2, width // 2), F32),
            vmem((cols // 2, width // 2), F32),
            vmem((cols // 2, width // 2), BF16),
            vmem((2, width, cols), BF16),
            vmem((2, 4, cols, tokens // 4), BF16),
            vmem((2, 4, cols, tokens // 4), BF16),
            vmem((cols, tokens), BF16),
            vmem((5, 8, 128), F32),
            vmem((3, 8, 128), F32),
            vmem((4, 8, 128), F32),
            vmem((4, 8, 128), F32),
            vmem((4, 8, 128), F32),
            pltpu.SemaphoreType.DMA((MESSAGES,)),
            pltpu.SemaphoreType.DMA((MESSAGES,)),
            pltpu.SemaphoreType.DMA((2,)),
        ],
        compiler_params=pltpu.CompilerParams(
            collective_id=0, has_side_effects=True, vmem_limit_bytes=51 * 1024 * 1024
        ),
    )(spans, states)


def solution(mesh):
    split = Mesh(mesh.devices.reshape(2, 2, 4, 4, 2), AXES)
    return jax.shard_map(
        per_device,
        mesh=split,
        in_specs=(P(SECTION, TOK, None), P()),
        out_specs=(P(None, SECTION, TOK), P(None, SECTION, TOK)),
        check_vma=False,
    )
```
